32 devices in a mesh: groups: 2 (over x), tm: 8 (over z, y), rows: 2 (over core).
Axes of the slice: x: 2, y: 2, z: 4, core: 2. Of those that a mesh axis runs over, the one named last changes fastest.
Arguments:
- video_tokens: bfloat16 [32, 32, 32, 1152], P(('groups', 'tm'), 'rows'), parts along dimension 0, may hold values from -6 to 6
- conv_weight: bfloat16 [3, 3, 9, 128, 128], replicated, may hold values from -0.1875 to 0.1875
- point_weight: bfloat16 [1152, 1152], replicated, may hold values from -0.1875 to 0.1875
- depth_weight: bfloat16 [3, 3, 3, 1152], replicated, may hold values from -1.25 to 1.25
- proj_weight: bfloat16 [1152, 8192], P(('tm', 'rows')), may hold values from -0.1875 to 0.1875
- rank_order: int32 [32], P('groups'), parts along dimension 0, may hold values from 0 to 15, each once
Outputs:
- llm_tokens: bfloat16 [4096, 8192], P(('groups', 'tm', 'rows')), parts along dimension 0
The draws below stay inside these ranges and needn't reach their ends.
There are 2 independent parts, one for each index of `groups`. The reference program is written for one: setup_inputs(seed, part) draws one part's arguments, and reference() takes and returns one part's arrays. A program takes and returns all parts, laid end to end along the dimension named above; an argument that names none is the same for every part. Nothing has to cross between parts.
Inputs may be any that keep to these rules, and one draw needn't show every extreme that they name: `rank_order`: each of 0 to 15 appears once.
All inputs are finite; a program needn't handle non-finite values.
Results may differ from the reference program's by a relative error of at most 0.0062.
Values may be sent and summed in bfloat16 or wider, within the bound.
No kernel may reach another device: no remote copies, remote signals or barrier semaphores. Data moves between devices by JAX's collectives and lax.ppermute only.
A program may use at most 192 MiB of HBM per device.

```python
import jax
import jax.numpy as jnp
from jax import lax

C = 1152
D = 8192
GW = 128
H = 32
W = 32
GROUPS = 9
FRAMES = 16
RANKS = 16
N_TM = 8
N_ROWS = 2


def levels(stream_key, shape, shards, low, largest):
    factor_of, own = 1.0, jax.random.fold_in(stream_key, 6)
    for axis_at, blocks in shards:
        draws = jnp.exp(jax.random.uniform(jax.random.fold_in(own, axis_at), (blocks,), jnp.float32, low / len(shards), largest / len(shards)))
        factor_of = factor_of * jnp.repeat(draws, shape[axis_at] // blocks).reshape([-1 if axis == axis_at else 1 for axis in range(len(shape))])
    return factor_of


def noise(key, extent, scale, bound, cuts=(), kind=jnp.bfloat16):
    values = scale * jax.random.normal(key, extent, jnp.float32)
    if cuts:
        values = values * levels(key, extent, cuts, -0.22, 0.18)
    return jnp.clip(values, -bound, bound).astype(kind)


def setup_inputs(seed: int = 0, part: int = 0) -> dict:
    key_of = jax.random.split(jax.random.key(seed), 7)
    part_splits = jax.random.split(jax.random.fold_in(key_of[6], part), 7)
    video_tokens = noise(part_splits[0], (FRAMES, H, W, C), 1.0, 6.0, ((0, 8), (1, 2)))
    conv_weight = noise(key_of[1], (3, 3, GROUPS, GW, GW), (9 * GW) ** -0.5, 0.1875)
    point_weight = noise(key_of[2], (C, C), C ** -0.5, 0.1875)
    depth_weight = noise(key_of[3], (3, 3, 3, C), 27 ** -0.5, 1.25)
    proj_weight = noise(key_of[4], (C, D), C ** -0.5, 0.1875, ((0, 16),))
    rank_order = jax.random.permutation(part_splits[5], RANKS).astype(jnp.int32)
    return {"video_tokens": video_tokens, "conv_weight": conv_weight, "point_weight": point_weight, "depth_weight": depth_weight, "proj_weight": proj_weight, "rank_order": rank_order}


def layer_norm(values):
    average = lax.optimization_barrier(jnp.mean(values, axis=-1, keepdims=True))
    spread = lax.optimization_barrier(jnp.mean(jnp.square(values - average), axis=-1, keepdims=True))
    return (values - average) * lax.rsqrt(spread + 1e-05)

def reference(video_tokens, conv_weight, point_weight, depth_weight, proj_weight, rank_order):
    frames, height, across, channels = video_tokens.shape
    group_count = channels // GW
    padded = jnp.pad(video_tokens, ((0, 0), (1, 1), (1, 1), (0, 0)))
    convolved = jnp.zeros((frames, height, across, channels), jnp.float32)
    for tap_row in range(3):
        for tap_col in range(3):
            window_cells = padded[:, tap_row:tap_row + height, tap_col:tap_col + across].astype(jnp.float32)
            window_cells = window_cells.reshape(frames, height, across, group_count, GW)
            product = jnp.einsum('fhwgi,gio->fhwgo', window_cells, conv_weight[tap_row, tap_col].astype(jnp.float32))
            convolved = convolved + product.reshape(frames, height, across, channels)
    activated = jax.nn.silu(layer_norm(convolved)).astype(jnp.bfloat16)
    mixed_branch = layer_norm(jnp.dot(activated.reshape(-1, channels), point_weight, preferred_element_type=jnp.float32))
    mixed_branch = mixed_branch.reshape(frames, height, across, channels)
    block_out = jax.nn.silu(video_tokens.astype(jnp.float32) + mixed_branch).astype(jnp.bfloat16)
    padded_block = jnp.pad(block_out, ((1, 0), (1, 0), (1, 0), (0, 0)))
    out_frames, out_rows, out_cols = (frames // 2, height // 2, across // 2)
    sampled = jnp.zeros((out_frames, out_rows, out_cols, channels), jnp.float32)
    for tap_time in range(3):
        for tap_row in range(3):
            for tap_col in range(3):
                taken = padded_block[tap_time:tap_time + 2 * out_frames - 1:2, tap_row:tap_row + 2 * out_rows - 1:2, tap_col:tap_col + 2 * out_cols - 1:2]
                sampled = sampled + depth_weight[tap_time, tap_row, tap_col].astype(jnp.float32) * taken.astype(jnp.float32)
    tokens = jax.nn.silu(sampled).astype(jnp.bfloat16).reshape(-1, channels)
    projected = jnp.dot(tokens, proj_weight, preferred_element_type=jnp.float32).astype(jnp.bfloat16)
    seq_len = tokens.shape[0]
    rank_count = N_TM * N_ROWS
    position = jnp.arange(seq_len, dtype=jnp.int32)
    stripe_class = position % (2 * rank_count)
    folded = jnp.minimum(stripe_class, 2 * rank_count - 1 - stripe_class)
    owners = rank_order[folded].astype(jnp.int32)
    ordering = jnp.argsort((owners * seq_len + position).astype(jnp.int32))
    return projected[ordering]
```

```python
import itertools

import jax
import jax.numpy as jnp
from jax import lax
from jax.sharding import PartitionSpec as P

AXES = ("groups", "tm", "rows")


def padded_2(cells, sides, width):
    for axis, dim in sides:
        count = lax.axis_size(axis)
        ends = count - 1
        head = lax.slice_in_dim(cells, 0, width, axis=dim)
        tail = lax.slice_in_dim(cells, cells.shape[dim] - width, cells.shape[dim], axis=dim)
        cells = jnp.concatenate(
            [
                lax.ppermute(tail, axis, [(i, (i + 1) % count) for i in range(ends)]),
                cells,
                lax.ppermute(head, axis, [((i + 1) % count, i) for i in range(ends)]),
            ],
            axis=dim,
        )
    return cells


def passed_along(value, axis, steps):
    count = lax.axis_size(axis)
    initial, last = (max(0, -steps), min(count, count - steps))
    return lax.ppermute(value, axis, [(source, source + steps) for source in range(initial, last)])


def layer_norm(values):
    average = jnp.mean(values, axis=-1, keepdims=True)
    spread = jnp.mean(jnp.square(values - average), axis=-1, keepdims=True)
    return (values - average) * lax.rsqrt(spread + 1e-05)


def axes_of():
    groups, count, cores = (lax.axis_size(a) for a in AXES)
    inner = 2 if count % 2 == 0 else 1
    return groups, count // inner, inner, cores


def place_of():
    groups, outer, inner, cores = axes_of()
    along = lax.axis_index("tm")
    return lax.axis_index("groups"), along // inner, along % inner, lax.axis_index("rows")


def shifted(value, steps):
    sizes = axes_of()
    if not any(steps):
        return value
    pairs = []
    for source, here in enumerate(itertools.product(*(range(n) for n in sizes))):
        there = [(a + b) % n for a, b, n in zip(here, steps, sizes)]
        target = 0
        for a, n in zip(there, sizes):
            target = target * n + a
        pairs.append((source, target))
    return lax.ppermute(value, AXES, pairs)


def spread_weight(proj_weight):
    groups, outer, inner, cores = axes_of()
    g, z, y, c = place_of()
    depth, width = proj_weight.shape
    block = width // (groups * inner * cores)
    level = jnp.zeros((inner * cores, depth, block), proj_weight.dtype)
    for dy, dc in itertools.product(range(inner), range(cores)):
        to = (g * inner + (y + dy) % inner) * cores + (c + dc) % cores
        piece = lax.dynamic_slice_in_dim(proj_weight, to * block, block, axis=1)
        piece = shifted(piece, (0, 0, dy, dc))
        source = ((y - dy) % inner) * cores + (c - dc) % cores
        level = lax.dynamic_update_slice_in_dim(level, piece[None], source, axis=0)
    level = level.reshape(1, inner * cores * depth, block)
    whole = jnp.zeros((outer,) + level.shape[1:], level.dtype)
    for dz in range(outer):
        piece = shifted(level, (0, dz, 0, 0))
        whole = lax.dynamic_update_slice_in_dim(whole, piece, (z - dz) % outer, axis=0)
    return whole.reshape(-1, block)


def deliver(tokens, rank_order, weight):
    groups, outer, inner, cores = axes_of()
    g, z, y, c = place_of()
    count, channels = tokens.shape
    ranks = outer * inner * cores
    period = 2 * ranks
    share = count // ranks
    position = jnp.arange(count, dtype=jnp.int32)
    stripe = position % period
    owner = rank_order[jnp.minimum(stripe, period - 1 - stripe)]
    target = owner * share + (position // period) * 2 + (stripe >= ranks).astype(jnp.int32)
    selector = (target[None, :] == position[:, None]).astype(jnp.bfloat16)
    placed = jnp.dot(selector, tokens, preferred_element_type=jnp.float32).astype(jnp.bfloat16)
    placed = placed.reshape(outer, inner * cores * share, channels)
    mine = jnp.zeros_like(placed)
    for dz in range(outer):
        piece = lax.dynamic_slice_in_dim(placed, (z + dz) % outer, 1, axis=0)
        piece = shifted(piece, (0, dz, 0, 0))
        mine = lax.dynamic_update_slice_in_dim(mine, piece, (z - dz) % outer, axis=0)
    chips = jnp.zeros((groups, inner) + mine.shape, mine.dtype)
    for dg, dy in itertools.product(range(groups), range(inner)):
        piece = shifted(mine, (dg, 0, dy, 0))[None, None]
        chips = lax.dynamic_update_slice(chips, piece, ((g - dg) % groups, (y - dy) % inner, 0, 0, 0))
    every = jnp.zeros((groups, inner, cores) + mine.shape, mine.dtype)
    for dc in range(cores):
        piece = shifted(chips, (0, 0, 0, dc))[:, :, None]
        every = lax.dynamic_update_slice(every, piece, (0, 0, (c - dc) % cores, 0, 0, 0))
    every = every.reshape(groups, inner * cores, outer, inner * cores, share, channels)
    every = jnp.transpose(every, (0, 3, 2, 1, 4, 5))
    peers = groups * inner * cores
    product = jnp.dot(every.reshape(-1, channels), weight, preferred_element_type=jnp.float32)
    product = product.astype(jnp.bfloat16).reshape(peers, count, -1)
    block = product.shape[2]
    out = jnp.zeros((count, peers * block), product.dtype)
    for dg, dy, dc in itertools.product(range(groups), range(inner), range(cores)):
        to = (((g + dg) % groups) * inner + (y + dy) % inner) * cores + (c + dc) % cores
        piece = lax.dynamic_index_in_dim(product, to, axis=0, keepdims=False)
        piece = shifted(piece, (dg, 0, dy, dc))
        source = (((g - dg) % groups) * inner + (y - dy) % inner) * cores + (c - dc) % cores
        out = lax.dynamic_update_slice_in_dim(out, piece, source * block, axis=1)
    return out


def three_taps(values, axis):
    length = values.shape[axis] - 1
    lower = lax.slice_in_dim(values, 0, length, axis=axis)
    upper = lax.slice_in_dim(values, 1, length + 1, axis=axis)
    new_shape = lower.shape[:axis] + (length // 2, 2) + lower.shape[axis + 1 :]
    lower = lower.reshape(new_shape)
    upper = upper.reshape(new_shape)
    first = lax.index_in_dim(lower, 0, axis + 1, keepdims=False)
    middle = lax.index_in_dim(upper, 0, axis + 1, keepdims=False)
    last = lax.index_in_dim(upper, 1, axis + 1, keepdims=False)
    return (first, middle, last)


def local(video_tokens, conv_weight, point_weight, depth_weight, proj_weight, rank_order):
    weight = spread_weight(proj_weight)
    frames, height, across, channels = video_tokens.shape
    group_width = conv_weight.shape[3]
    group_count = channels // group_width
    padded = padded_2(video_tokens, (("rows", 1),), 1)
    flat_cells = padded.reshape(-1, channels)
    group_outs = []
    for group in range(group_count):
        inputs = flat_cells[:, group * group_width : (group + 1) * group_width]
        taps_weight = jnp.transpose(conv_weight[:, :, group], (2, 0, 1, 3)).reshape(
            group_width, 9 * group_width
        )
        every_tap = jnp.dot(inputs, taps_weight, preferred_element_type=jnp.float32)
        every_tap = every_tap.reshape(frames, height + 2, across, 9 * group_width)
        column_sums = []
        for tap_col in range(3):
            total = None
            for tap_row in range(3):
                lane = (3 * tap_row + tap_col) * group_width
                piece = every_tap[:, tap_row : tap_row + height, :, lane : lane + group_width]
                total = piece if total is None else total + piece
            column_sums.append(total)
        left_part = jnp.pad(column_sums[0], ((0, 0), (0, 0), (1, 0), (0, 0)))[:, :, :across]
        right_part = jnp.pad(column_sums[2], ((0, 0), (0, 0), (0, 1), (0, 0)))[:, :, 1:]
        group_outs.append(column_sums[1] + left_part + right_part)
    convolved = jnp.concatenate(group_outs, axis=3)
    activated = jax.nn.silu(layer_norm(convolved)).astype(jnp.bfloat16)
    mixed_branch = layer_norm(
        jnp.dot(activated.reshape(-1, channels), point_weight, preferred_element_type=jnp.float32)
    )
    mixed_branch = mixed_branch.reshape(frames, height, across, channels)
    block_out = jax.nn.silu(video_tokens.astype(jnp.float32) + mixed_branch).astype(jnp.bfloat16)
    above_row = passed_along(block_out[:, -1:], "rows", 1)
    extended = jnp.concatenate([above_row, block_out], axis=1)
    prior_frame = passed_along(extended[-1:], "tm", 1)
    with_rims = jnp.concatenate([prior_frame, extended], axis=0)
    out_frames, out_rows, out_cols = (frames // 2, height // 2, across // 2)
    with_rims = with_rims.reshape(frames + 1, height + 1, out_cols, 2 * channels)
    time_taps = three_taps(with_rims, 0)
    depth_float = depth_weight.astype(jnp.float32)
    acc_left = jnp.zeros((out_frames, out_rows, out_cols, channels), jnp.float32)
    acc_mid = jnp.zeros((out_frames, out_rows, out_cols, channels), jnp.float32)
    acc_right = jnp.zeros((out_frames, out_rows, out_cols, channels), jnp.float32)
    for tap_time in range(3):
        row_taps = three_taps(time_taps[tap_time], 1)
        for tap_row in range(3):
            base = row_taps[tap_row]
            even_cols = base[..., :channels].astype(jnp.float32)
            odd_cols = base[..., channels:].astype(jnp.float32)
            acc_left = acc_left + depth_float[tap_time, tap_row, 0] * odd_cols
            acc_mid = acc_mid + depth_float[tap_time, tap_row, 1] * even_cols
            acc_right = acc_right + depth_float[tap_time, tap_row, 2] * odd_cols
    shifted_left = jnp.pad(acc_left, ((0, 0), (0, 0), (1, 0), (0, 0)))[:, :, :out_cols]
    sampled = acc_mid + acc_right + shifted_left
    tokens = jax.nn.silu(sampled).astype(jnp.bfloat16).reshape(-1, channels)
    return deliver(tokens, rank_order, weight)


def solution(mesh):
    return jax.shard_map(
        local,
        mesh=mesh,
        in_specs=(
            P(("groups", "tm"), "rows", None, None),
            P(),
            P(),
            P(),
            P(("tm", "rows"), None),
            P("groups"),
        ),
        out_specs=P(("groups", "tm", "rows"), None),
        check_vma=False,
    )
```

```python
import itertools
import math

import jax
import jax.numpy as jnp
from jax import lax
from jax.experimental import pallas as pl
from jax.experimental.pallas import tpu as pltpu
from jax.sharding import PartitionSpec as P

AXES = ("groups", "tm", "rows")
SPREAD = 2


def axes_of():
    groups, count, cores = (lax.axis_size(a) for a in AXES)
    inner = math.gcd(count, SPREAD)
    return groups, count // inner, inner, cores


def place_of():
    _, _, inner, _ = axes_of()
    along = lax.axis_index("tm")
    return lax.axis_index("groups"), along // inner, along % inner, lax.axis_index("rows")


def shifted(value, steps):
    sizes = axes_of()
    if not any(steps):
        return value
    pairs = []
    for source, here in enumerate(itertools.product(*(range(n) for n in sizes))):
        there = [(a + b) % n for a, b, n in zip(here, steps, sizes)]
        target = 0
        for a, n in zip(there, sizes):
            target = target * n + a
        pairs.append((source, target))
    return lax.ppermute(value, AXES, pairs)


def silu(values):
    half = 0.5 * values
    return half + half * jnp.tanh(half)


def normal(values):
    scale = 1.0 / values.shape[-1]
    centred = values - jnp.sum(values, axis=-1, keepdims=True) * scale
    spread = jnp.sum(centred * centred, axis=-1, keepdims=True) * scale
    return centred * lax.rsqrt(spread + 1e-05)


def block_kernel(frame, planes, first, refs):
    if first:
        (above_ok, x_hbm, up_hbm, down_hbm, conv_hbm, point_hbm, depth_ref, sent_ref, kept_ref,
         xin, xl, xr, conv_v, point_v, wide, act, rim, sems, conv_sems) = refs
        start_ref, out_refs = None, (sent_ref, kept_ref)
    else:
        (above_ok, x_hbm, up_hbm, down_hbm, conv_hbm, point_hbm, depth_ref, start_ref, kept_ref,
         xin, xl, xr, conv_v, point_v, wide, act, rim, sems, conv_sems) = refs
        out_refs = (kept_ref,)
    pairs, _, across, channels = xin.shape
    width = conv_v.shape[-1]
    groups = channels // width
    copies = [
        pltpu.make_async_copy(x_hbm.at[frame], xin.at[pl.ds(1, pairs - 2)], sems.at[0]),
        pltpu.make_async_copy(up_hbm.at[frame], xin.at[0], sems.at[1]),
        pltpu.make_async_copy(down_hbm.at[frame], xin.at[pairs - 1], sems.at[2]),
    ]

    def conv_copy(g):
        return pltpu.make_async_copy(conv_hbm.at[:, :, g], conv_v.at[:, :, g], conv_sems.at[g])

    point_copy = pltpu.make_async_copy(point_hbm, point_v, sems.at[3])
    for copy in copies + [conv_copy(g) for g in range(groups)] + [point_copy]:
        copy.start()
    for copy in copies:
        copy.wait()

    column = lax.broadcasted_iota(jnp.int32, (across, channels), 0)

    def shift(i, carry):
        k, p = i // 2, i % 2
        row = xin[k, p].astype(jnp.float32)
        left = jnp.where(column == 0, 0.0, pltpu.roll(row, 1, 0))
        right = jnp.where(column == across - 1, 0.0, pltpu.roll(row, across - 1, 0))
        xl[k, p] = left.astype(jnp.bfloat16)
        xr[k, p] = right.astype(jnp.bfloat16)
        return carry

    lax.fori_loop(0, 2 * pairs, shift, 0)

    span = pairs - 1
    order = []
    for half in (0, 2):
        order += [(half, 0), (half, 1), (half + 1, 0), (half + 1, 1), (half, 2), (half + 1, 2)]
    sources = (xl, xin, xr)
    zero = jnp.zeros((width, width), jnp.bfloat16)

    def convolve(g, carry):
        lanes = pl.ds(pl.multiple_of(g * width, width), width)
        conv_copy(g).wait()
        left_side, right_side = [], []
        for a, b in order:
            piece = sources[b][pl.ds(a // 2, span), a % 2, :, lanes]
            left_side.append(piece.reshape(span * across, width))
            taps = [conv_v[a - j, b, g] if 0 <= a - j < 3 else zero for j in range(2)]
            right_side.append(jnp.concatenate(taps, axis=1))
        out = jnp.dot(
            jnp.concatenate(left_side, axis=1),
            jnp.concatenate(right_side, axis=0),
            preferred_element_type=jnp.float32,
        )
        for j in range(2):
            wide[:, j, :, lanes] = out[:, j * width : (j + 1) * width].reshape(span, across, width)
        return carry

    lax.fori_loop(0, groups, convolve, 0)

    def activate(i, carry):
        for p in range(2):
            for h in range(0, across, 16):
                act[i, p, pl.ds(h, 16)] = silu(normal(wide[i, p, pl.ds(h, 16)])).astype(jnp.bfloat16)
        return carry

    lax.fori_loop(0, span, activate, 0)
    point_copy.wait()
    step = 2 * width

    def mix(at, lanes):
        product = jnp.dot(
            act[...].reshape(2 * span * across, channels),
            point_v[:, lanes],
            preferred_element_type=jnp.float32,
        )
        wide[:, :, :, lanes] = product.reshape(span, 2, across, product.shape[1])
        return at

    lax.fori_loop(0, channels // step, lambda n, t: mix(t, pl.ds(pl.multiple_of(n * step, step), step)), 0)
    if channels % step:
        mix(0, pl.ds(channels // step * step, channels % step))

    margin = rim.shape[2] - across
    keep = above_ok[0].astype(jnp.float32)

    def finish(i, carry):
        for p in range(2):
            for h in range(0, across, 16):
                value = xin[i + p, 1 - p, pl.ds(h, 16)].astype(jnp.float32)
                value = silu(value + normal(wide[i, p, pl.ds(h, 16)]))
                if p == 0:
                    value = jnp.where(i == 0, value * keep, value)
                for g in range(groups):
                    rim[g, 2 * i + p, pl.ds(margin + h, 16), :] = value[:, g * width : (g + 1) * width]
            for g in range(groups):
                rim[g, 2 * i + p, pl.ds(0, margin), :] = jnp.zeros((margin, width), jnp.float32)
        return carry

    lax.fori_loop(0, span, finish, 0)

    half = across // 2

    def sample_group(g, outer):
        lanes = pl.ds(pl.multiple_of(g * width, width), width)
        weights = [
            [
                jnp.broadcast_to(depth_ref[pl.ds(plane * 9 + tap, 1), lanes].astype(jnp.float32), (8, width))
                for tap in range(9)
            ]
            for plane in planes
        ]

        def sample(p, carry):
            for t in range(half // 8):
                where = pl.ds(pl.multiple_of(p * half + 8 * t, 8), 8)
                totals = [None] * len(planes)
                if start_ref is not None:
                    totals[0] = start_ref[where, lanes]
                for b in range(3):
                    for e in range(3):
                        value = rim[g, 2 * p + b, pl.ds(margin - 1 + e + 16 * t, 8, 2), :]
                        for n in range(len(planes)):
                            term = weights[n][3 * b + e] * value
                            totals[n] = term if totals[n] is None else totals[n] + term
                for ref, total in zip(out_refs, totals):
                    ref[where, lanes] = total
            return carry

        lax.fori_loop(0, span - 1, sample, 0, unroll=2)
        return outer

    lax.fori_loop(0, groups, sample_group, 0)


def block_call(frame, above_ok, x, up, down, conv_weight, point_weight, depth_weight, start=None):
    first = start is None
    _, near, _, across, channels = x.shape
    pairs = near + 2
    span = pairs - 1
    groups, width = conv_weight.shape[2:4]
    count = near * (across // 2)
    out = jax.ShapeDtypeStruct((count, channels), jnp.float32)
    anywhere = pl.BlockSpec(memory_space=pltpu.HBM)
    vmem = pl.BlockSpec(memory_space=pltpu.VMEM)
    args = [above_ok, x, up, down, conv_weight, point_weight, depth_weight] + ([] if first else [start])
    planes = (0, 2) if first else (1,)
    return pl.pallas_call(
        lambda *refs: block_kernel(frame, planes, first, refs),
        out_shape=[out, out] if first else out,
        in_specs=[pl.BlockSpec(memory_space=pltpu.SMEM)] + [anywhere] * 5 + [vmem] * (1 if first else 2),
        out_specs=[vmem, vmem] if first else vmem,
        scratch_shapes=[
            pltpu.VMEM((pairs, 2, across, channels), jnp.bfloat16),
            pltpu.VMEM((pairs, 2, across, channels), jnp.bfloat16),
            pltpu.VMEM((pairs, 2, across, channels), jnp.bfloat16),
            pltpu.VMEM(conv_weight.shape, jnp.bfloat16),
            pltpu.VMEM(point_weight.shape, jnp.bfloat16),
            pltpu.VMEM((span, 2, across, channels), jnp.float32),
            pltpu.VMEM((span, 2, across, channels), jnp.bfloat16),
            pltpu.VMEM((groups, 2 * span, across + 8, width), jnp.float32),
            pltpu.SemaphoreType.DMA((4,)),
            pltpu.SemaphoreType.DMA((groups,)),
        ],
        compiler_params=pltpu.CompilerParams(vmem_limit_bytes=62 << 20),
        name="block_last" if first else "block_first",
    )(*args)


HBM = pl.BlockSpec(memory_space=pltpu.HBM)
VMEM = pl.BlockSpec(memory_space=pltpu.VMEM)
SMEM = pl.BlockSpec(memory_space=pltpu.SMEM)


def run_copies(copies):
    for copy in copies:
        copy.start()
    for copy in copies:
        copy.wait()


def cut_kernel(weight_ref, *refs):
    _, _, inner, cores = axes_of()
    g, _, y, c = place_of()
    pieces, sem = refs[:-1], refs[-1]
    block = pieces[0].shape[1]
    copies = []
    for n, (dy, dc) in enumerate(itertools.product(range(inner), range(cores))):
        to = (g * inner + lax.rem(y + dy, inner)) * cores + lax.rem(c + dc, cores)
        lanes = pl.ds(pl.multiple_of(to * block, 128), block)
        copies.append(pltpu.make_async_copy(weight_ref.at[:, lanes], pieces[n], sem.at[n]))
    run_copies(copies)


def join_kernel(*refs):
    _, _, inner, cores = axes_of()
    _, _, y, c = place_of()
    pieces, level_ref = refs[:-1], refs[-1]
    depth = pieces[0].shape[0]
    for n, (dy, dc) in enumerate(itertools.product(range(inner), range(cores))):
        source = lax.rem(y + inner - dy, inner) * cores + lax.rem(c + cores - dc, cores)
        level_ref[pl.ds(pl.multiple_of(source * depth, 8), depth), :] = pieces[n][...]


def spread_weight(proj_weight):
    groups, outer, inner, cores = axes_of()
    g, _, y, c = place_of()
    depth, width = proj_weight.shape
    block = width // (groups * inner * cores)
    steps = list(itertools.product(range(inner), range(cores)))
    to = [(g * inner + (y + dy) % inner) * cores + (c + dc) % cores for dy, dc in steps]
    source = [((y - dy) % inner) * cores + (c - dc) % cores for dy, dc in steps]
    aligned = depth % 8 == 0 and block % 128 == 0
    shape = jax.ShapeDtypeStruct((depth, block), proj_weight.dtype)
    if aligned:
        pieces = pl.pallas_call(
            cut_kernel,
            out_shape=[shape] * len(steps),
            in_specs=[HBM],
            out_specs=[VMEM] * len(steps),
            scratch_shapes=[pltpu.SemaphoreType.DMA((len(steps),))],
            compiler_params=pltpu.CompilerParams(vmem_limit_bytes=8 << 20),
            name="cut",
        )(proj_weight)
    else:
        pieces = [lax.dynamic_slice_in_dim(proj_weight, t * block, block, axis=1) for t in to]
    pieces = [shifted(piece, (0, 0, dy, dc)) for piece, (dy, dc) in zip(pieces, steps)]
    rows = len(steps) * depth
    if aligned:
        level = pl.pallas_call(
            join_kernel,
            out_shape=jax.ShapeDtypeStruct((rows, block), proj_weight.dtype),
            in_specs=[VMEM] * len(steps),
            out_specs=VMEM,
            compiler_params=pltpu.CompilerParams(vmem_limit_bytes=8 << 20),
            name="join",
        )(*pieces)
    else:
        level = jnp.zeros((rows, block), proj_weight.dtype)
        for piece, at in zip(pieces, source):
            level = lax.dynamic_update_slice_in_dim(level, piece, at * depth, axis=0)
    count = lax.axis_size("tm")
    forward, backward = [level], [level]
    for _ in range(1, outer):
        forward.append(
            lax.ppermute(forward[-1], "tm", [(i, i + inner) for i in range(count - inner)])
        )
        backward.append(
            lax.ppermute(backward[-1], "tm", [(i + inner, i) for i in range(count - inner)])
        )
    return forward, backward


def project_kernel(outer, inner, cores, *refs):
    peers = inner * cores
    x_refs, refs = refs[:peers], refs[peers:]
    f_refs, refs = refs[:outer], refs[outer:]
    b_refs, refs = refs[: outer - 1], refs[outer - 1 :]
    out_refs, (xs, ws, product, x_sem, w_sem) = refs[:peers], refs[peers:]
    _, z, y, c = place_of()
    count = x_refs[0].shape[0]
    rows, block = f_refs[0].shape
    share = count // (outer * peers)
    for n, x_ref in enumerate(x_refs):
        pltpu.make_async_copy(x_ref, xs.at[pl.ds(n * count, count)], x_sem.at[n]).start()

    def into(step):
        source = lax.rem(z + outer - step, outer)
        return ws.at[pl.ds(pl.multiple_of(source * rows, 16), rows)]

    pltpu.make_async_copy(f_refs[0], into(0), w_sem.at[0]).start()
    for step in range(1, outer):

        @pl.when(z >= step)
        def _():
            pltpu.make_async_copy(f_refs[step], into(step), w_sem.at[step]).start()

        @pl.when(z < step)
        def _():
            pltpu.make_async_copy(b_refs[outer - step - 1], into(step), w_sem.at[step]).start()

    for n, x_ref in enumerate(x_refs):
        pltpu.make_async_copy(x_ref, xs.at[pl.ds(n * count, count)], x_sem.at[n]).wait()
    for step in range(outer):
        pltpu.make_async_copy(f_refs[step], into(step), w_sem.at[step]).wait()

    def multiply(n, carry):
        lanes = pl.ds(pl.multiple_of(n * 256, 256), 256)
        out = jnp.dot(xs[...], ws[:, lanes], preferred_element_type=jnp.float32)
        product[:, :, :, :, lanes] = out.reshape(peers, outer, peers, share, 256)
        return carry

    lax.fori_loop(0, block // 256, multiply, 0)
    for n, (ty, tc) in enumerate(itertools.product(range(inner), range(cores))):
        target = lax.rem(y + ty, inner) * cores + lax.rem(c + tc, cores)
        for dz, dy in itertools.product(range(outer), range(inner)):
            from_z, from_y = lax.rem(z + outer - dz, outer), lax.rem(y + inner - dy, inner)
            tiles = []
            for from_c in range(cores):
                dc = lax.rem(c + cores - from_c, cores)
                tiles.append(product[dy * cores + dc, dz, target])
            at = (from_z * inner + from_y) * cores * share
            tile = jnp.concatenate(tiles, axis=0).astype(jnp.bfloat16)
            out_refs[n][pl.ds(pl.multiple_of(at, cores * share), cores * share), :] = tile


def project_call(blocks, forward, backward, outer, inner, cores):
    peers = inner * cores
    count, channels = blocks[0].shape
    rows, block = forward[0].shape
    share = count // (outer * peers)
    vmem = pl.BlockSpec(memory_space=pltpu.VMEM)
    return pl.pallas_call(
        lambda *refs: project_kernel(outer, inner, cores, *refs),
        out_shape=[jax.ShapeDtypeStruct((count, block), jnp.bfloat16)] * peers,
        in_specs=[HBM] * (peers + 2 * outer - 1),
        out_specs=[vmem] * peers,
        scratch_shapes=[
            pltpu.VMEM((peers * count, channels), jnp.bfloat16),
            pltpu.VMEM((outer * rows, block), jnp.bfloat16),
            pltpu.VMEM((peers, outer, peers, share, block), jnp.float32),
            pltpu.SemaphoreType.DMA((peers,)),
            pltpu.SemaphoreType.DMA((outer,)),
        ],
        compiler_params=pltpu.CompilerParams(vmem_limit_bytes=32 << 20),
        name="project",
    )(*blocks, *forward, *backward)


def project_plain(blocks, forward, backward, outer, inner, cores):
    _, z, y, c = place_of()
    peers = inner * cores
    count, channels = blocks[0].shape
    block = forward[0].shape[1]
    share = count // (outer * peers)
    whole = jnp.zeros((outer,) + forward[0].shape, forward[0].dtype)
    for step in range(outer):
        piece = forward[step]
        if step:
            piece = jnp.where(z >= step, piece, backward[outer - step - 1])
        whole = lax.dynamic_update_slice_in_dim(whole, piece[None], (z - step) % outer, axis=0)
    every = jnp.zeros((inner, cores, outer, peers, share, channels), jnp.bfloat16)
    for n, (dy, dc) in enumerate(itertools.product(range(inner), range(cores))):
        piece = blocks[n].reshape(outer, peers, share, channels)
        piece = jnp.roll(piece[(-jnp.arange(outer)) % outer], z, axis=0)
        every = lax.dynamic_update_slice(
            every, piece[None, None], ((y - dy) % inner, (c - dc) % cores, 0, 0, 0, 0)
        )
    every = jnp.transpose(every, (3, 2, 0, 1, 4, 5)).reshape(-1, channels)
    product = jnp.dot(every, whole.reshape(-1, block), preferred_element_type=jnp.float32)
    product = product.astype(jnp.bfloat16).reshape(peers, count, block)
    return [
        lax.dynamic_index_in_dim(product, ((y + ty) % inner) * cores + (c + tc) % cores, 0, False)
        for ty, tc in itertools.product(range(inner), range(cores))
    ]


def collect_kernel(*refs):
    groups, _, inner, cores = axes_of()
    g, _, y, c = place_of()
    pieces, out_ref, sem = refs[:-2], refs[-2], refs[-1]
    block = pieces[0].shape[1]
    copies = []
    for n, (dg, dy, dc) in enumerate(itertools.product(range(groups), range(inner), range(cores))):
        source = lax.rem(g + groups - dg, groups) * inner + lax.rem(y + inner - dy, inner)
        source = source * cores + lax.rem(c + cores - dc, cores)
        lanes = pl.ds(pl.multiple_of(source * block, 128), block)
        copies.append(pltpu.make_async_copy(pieces[n], out_ref.at[:, lanes], sem.at[n]))
    run_copies(copies)


def deliver(placed, forward, backward):
    groups, outer, inner, cores = axes_of()
    g, _, y, c = place_of()
    count, _ = placed.shape
    block = forward[0].shape[1]
    part = count // outer
    share = part // (inner * cores)
    mine = [shifted(placed[dz * part : (dz + 1) * part], (0, dz, 0, 0)) for dz in range(outer)]
    mine = jnp.concatenate(mine, axis=0)
    chips = {}
    for dg, dy in itertools.product(reversed(range(groups)), reversed(range(inner))):
        chips[dg, dy] = shifted(mine, (dg, 0, dy, 0))
    blocks = {}
    for dg, dy, dc in itertools.product(range(groups), range(inner), range(cores)):
        blocks[dg, dy, dc] = shifted(chips[dg, dy], (0, 0, 0, dc))
    fits = cores * share % 16 == 0 and share % 8 == 0 and block % 256 == 0
    call = project_call if fits else project_plain
    steps = list(itertools.product(range(inner), range(cores)))
    arrived = {}
    for dg in reversed(range(groups)):
        group = [blocks[dg, dy, dc] for dy, dc in steps]
        pieces = call(group, forward, backward[1:], outer, inner, cores)
        for (dy, dc), piece in zip(steps, pieces):
            arrived[dg, dy, dc] = shifted(piece, (dg, 0, dy, dc))
    if fits:
        pieces = [piece for _, piece in sorted(arrived.items())]
        return pl.pallas_call(
            collect_kernel,
            out_shape=jax.ShapeDtypeStruct((count, len(pieces) * block), jnp.bfloat16),
            in_specs=[VMEM] * len(pieces),
            out_specs=HBM,
            scratch_shapes=[pltpu.SemaphoreType.DMA((len(pieces),))],
            compiler_params=pltpu.CompilerParams(vmem_limit_bytes=8 << 20),
            name="collect",
        )(*pieces)
    out = jnp.zeros((count, groups * inner * cores * block), jnp.bfloat16)
    for (dg, dy, dc), piece in sorted(arrived.items()):
        source = (((g - dg) % groups) * inner + (y - dy) % inner) * cores + (c - dc) % cores
        out = lax.dynamic_update_slice_in_dim(out, piece, source * block, axis=1)
    return out


def place_kernel(sum_ref, rim_ref, target_ref, placed_ref):
    count = sum_ref.shape[0]
    tokens = silu(sum_ref[...] + rim_ref[...].astype(jnp.float32)).astype(jnp.bfloat16)
    slot = lax.broadcasted_iota(jnp.int32, (count, count), 0)
    selector = jnp.where(slot == target_ref[...], 1.0, 0.0).astype(jnp.bfloat16)
    placed = jnp.dot(selector, tokens, preferred_element_type=jnp.float32)
    placed_ref[...] = placed.astype(jnp.bfloat16)


def place_call(total, rim, target):
    vmem = pl.BlockSpec(memory_space=pltpu.VMEM)
    return pl.pallas_call(
        place_kernel,
        out_shape=jax.ShapeDtypeStruct(total.shape, jnp.bfloat16),
        in_specs=[vmem] * 3,
        out_specs=vmem,
        compiler_params=pltpu.CompilerParams(vmem_limit_bytes=8 << 20),
        name="place",
    )(total, rim, target)


def slots(rank_order, count):
    _, outer, inner, cores = axes_of()
    _, z, _, _ = place_of()
    ranks = outer * inner * cores
    period = 2 * ranks
    share = count // ranks
    position = jnp.arange(count, dtype=jnp.int32)
    stripe = position % period
    folded = jnp.minimum(stripe, period - 1 - stripe)
    one_hot = folded[:, None] == jnp.arange(ranks, dtype=jnp.int32)[None, :]
    owner = jnp.sum(jnp.where(one_hot, rank_order[None, :], 0), axis=1)
    owner = (owner + (outer - z) * inner * cores) % ranks
    target = owner * share + (position // period) * 2 + (stripe >= ranks).astype(jnp.int32)
    return target.reshape(1, count)


def local(video_tokens, conv_weight, point_weight, depth_weight, proj_weight, rank_order):
    frames, height, across, channels = video_tokens.shape
    forward, backward = spread_weight(proj_weight)
    cores = lax.axis_size("rows")
    up = lax.ppermute(video_tokens[:, -2:], "rows", [(i, i + 1) for i in range(cores - 1)])
    down = lax.ppermute(video_tokens[:, :2], "rows", [(i + 1, i) for i in range(cores - 1)])
    paired = video_tokens.reshape(frames, height // 2, 2, across, channels)
    taps = depth_weight.reshape(-1, channels).astype(jnp.float32)
    above_ok = (lax.axis_index("rows") > 0).astype(jnp.int32).reshape(1)
    shared = (above_ok, paired, up, down, conv_weight, point_weight, taps)
    along = lax.axis_size("tm")
    sums, rims = [], []
    for o in reversed(range(frames // 2)):
        sent, kept = block_call(2 * o + 1, *shared)
        rims.insert(0, sent)
        sums.insert(0, block_call(2 * o, *shared, kept))
    rim = lax.ppermute(rims[-1].astype(jnp.bfloat16), "tm", [(i, i + 1) for i in range(along - 1)])
    if frames > 2:
        rim = jnp.concatenate([rim.astype(jnp.float32)] + rims[:-1], axis=0)
    total = sums[0] if len(sums) == 1 else jnp.concatenate(sums, axis=0)
    placed = place_call(total, rim, slots(rank_order, total.shape[0]))
    return deliver(placed, forward, backward)


def solution(mesh):
    return jax.shard_map(
        local,
        mesh=mesh,
        in_specs=(
            P(("groups", "tm"), "rows", None, None),
            P(),
            P(),
            P(),
            P(("tm", "rows"), None),
            P("groups"),
        ),
        out_specs=P(("groups", "tm", "rows"), None),
        check_vma=False,
    )
```

```python
import itertools
import math

import jax
import jax.numpy as jnp
from jax import lax
from jax.experimental import pallas as pl
from jax.experimental.pallas import tpu as pltpu
from jax.sharding import PartitionSpec as P

AXES = ("groups", "tm", "rows")
SPREAD = 2
CHUNKS = 2


def axes_of():
    groups, count, cores = (lax.axis_size(a) for a in AXES)
    inner = math.gcd(count, SPREAD)
    return groups, count // inner, inner, cores


def place_of():
    _, _, inner, _ = axes_of()
    along = lax.axis_index("tm")
    return lax.axis_index("groups"), along // inner, along % inner, lax.axis_index("rows")


def shifted(value, steps):
    sizes = axes_of()
    if not any(steps):
        return value
    pairs = []
    for source, here in enumerate(itertools.product(*(range(n) for n in sizes))):
        there = [(a + b) % n for a, b, n in zip(here, steps, sizes)]
        target = 0
        for a, n in zip(there, sizes):
            target = target * n + a
        pairs.append((source, target))
    return lax.ppermute(value, AXES, pairs)


def silu(values):
    half = 0.5 * values
    return half + half * jnp.tanh(half)


def normal(values):
    scale = 1.0 / values.shape[-1]
    centred = values - jnp.sum(values, axis=-1, keepdims=True) * scale
    spread = jnp.sum(centred * centred, axis=-1, keepdims=True) * scale
    return centred * lax.rsqrt(spread + 1e-05)


def block_kernel(frame, planes, first, refs):
    if first:
        (x_hbm, up_ref, down_ref, conv_hbm, point_hbm, depth_ref, sent_ref, kept_ref,
         xin, xl, xr, conv_v, point_v, wide, act, rim, sems, conv_sems) = refs
        start_ref, out_refs = None, (sent_ref, kept_ref)
    else:
        (x_hbm, up_ref, down_ref, conv_hbm, point_hbm, depth_ref, start_ref, kept_ref,
         xin, xl, xr, conv_v, point_v, wide, act, rim, sems, conv_sems) = refs
        out_refs = (kept_ref,)
    pairs, _, across, channels = xin.shape
    width = conv_v.shape[-1]
    groups = channels // width
    copies = [
        pltpu.make_async_copy(x_hbm.at[frame], xin.at[pl.ds(1, pairs - 2)], sems.at[0]),
    ]

    def conv_copy(g):
        return pltpu.make_async_copy(conv_hbm.at[:, :, g], conv_v.at[:, :, g], conv_sems.at[g])

    point_copy = pltpu.make_async_copy(point_hbm, point_v, sems.at[3])
    for copy in copies + [conv_copy(g) for g in range(groups)] + [point_copy]:
        copy.start()
    for copy in copies:
        copy.wait()
    core, cores = lax.axis_index("rows"), lax.axis_size("rows")
    blank = jnp.zeros(xin.shape[1:], jnp.bfloat16)
    xin[0] = jnp.where(core == 0, blank, up_ref[frame])
    xin[pairs - 1] = jnp.where(core == cores - 1, blank, down_ref[frame])
    column = lax.broadcasted_iota(jnp.int32, (across, channels), 0)

    def shift(i, carry):
        k, p = i // 2, i % 2
        row = xin[k, p].astype(jnp.float32)
        left = jnp.where(column == 0, 0.0, pltpu.roll(row, 1, 0))
        right = jnp.where(column == across - 1, 0.0, pltpu.roll(row, across - 1, 0))
        xl[k, p] = left.astype(jnp.bfloat16)
        xr[k, p] = right.astype(jnp.bfloat16)
        return carry

    lax.fori_loop(0, 2 * pairs, shift, 0)

    span = pairs - 1
    order = []
    for half in (0, 2):
        order += [(half, 0), (half, 1), (half + 1, 0), (half + 1, 1), (half, 2), (half + 1, 2)]
    sources = (xl, xin, xr)
    zero = jnp.zeros((width, width), jnp.bfloat16)

    def convolve(g, carry):
        lanes = pl.ds(pl.multiple_of(g * width, width), width)
        conv_copy(g).wait()
        left_side, right_side = [], []
        for a, b in order:
            piece = sources[b][pl.ds(a // 2, span), a % 2, :, lanes]
            left_side.append(piece.reshape(span * across, width))
            taps = [conv_v[a - j, b, g] if 0 <= a - j < 3 else zero for j in range(2)]
            right_side.append(jnp.concatenate(taps, axis=1))
        out = jnp.dot(
            jnp.concatenate(left_side, axis=1),
            jnp.concatenate(right_side, axis=0),
            preferred_element_type=jnp.float32,
        )
        for j in range(2):
            wide[:, j, :, lanes] = out[:, j * width : (j + 1) * width].reshape(span, across, width)
        return carry

    lax.fori_loop(0, groups, convolve, 0)

    def activate(i, carry):
        for p in range(2):
            for h in range(0, across, 16):
                act[i, p, pl.ds(h, 16)] = silu(normal(wide[i, p, pl.ds(h, 16)])).astype(jnp.bfloat16)
        return carry

    lax.fori_loop(0, span, activate, 0, unroll=3)
    point_copy.wait()
    step = 2 * width

    def mix(at, lanes):
        product = jnp.dot(
            act[...].reshape(2 * span * across, channels),
            point_v[:, lanes],
            preferred_element_type=jnp.float32,
        )
        wide[:, :, :, lanes] = product.reshape(span, 2, across, product.shape[1])
        return at

    lax.fori_loop(0, channels // step, lambda n, t: mix(t, pl.ds(pl.multiple_of(n * step, step), step)), 0, unroll=True)
    if channels % step:
        mix(0, pl.ds(channels // step * step, channels % step))

    margin = rim.shape[2] - across
    keep = jnp.where(core == 0, 0.0, 1.0)

    def finish(i, carry):
        for p in range(2):
            for h in range(0, across, 16):
                value = xin[i + p, 1 - p, pl.ds(h, 16)].astype(jnp.float32)
                value = silu(value + normal(wide[i, p, pl.ds(h, 16)]))
                if p == 0:
                    value = jnp.where(i == 0, value * keep, value)
                for g in range(groups):
                    rim[g, 2 * i + p, pl.ds(margin + h, 16), :] = value[:, g * width : (g + 1) * width]
            for g in range(groups):
                rim[g, 2 * i + p, pl.ds(0, margin), :] = jnp.zeros((margin, width), jnp.float32)
        return carry

    lax.fori_loop(0, span, finish, 0, unroll=3)

    half = across // 2

    def sample_group(g, outer):
        lanes = pl.ds(pl.multiple_of(g * width, width), width)
        weights = [
            [
                jnp.broadcast_to(
                    depth_ref[plane, tap // 3, pl.ds(tap % 3, 1), lanes].astype(jnp.float32), (8, width)
                )
                for tap in range(9)
            ]
            for plane in planes
        ]

        def sample(p, carry):
            for t in range(half // 8):
                where = pl.ds(pl.multiple_of(p * half + 8 * t, 8), 8)
                totals = [None] * len(planes)
                if start_ref is not None:
                    totals[0] = start_ref[where, lanes]
                for b in range(3):
                    for e in range(3):
                        value = rim[g, 2 * p + b, pl.ds(margin - 1 + e + 16 * t, 8, 2), :]
                        for n in range(len(planes)):
                            term = weights[n][3 * b + e] * value
                            totals[n] = term if totals[n] is None else totals[n] + term
                for ref, total in zip(out_refs, totals):
                    ref[where, lanes] = total.astype(ref.dtype)
            return carry

        lax.fori_loop(0, span - 1, sample, 0, unroll=2)
        return outer

    lax.fori_loop(0, groups, sample_group, 0)


def block_call(frame, x, up, down, conv_weight, point_weight, depth_weight, start=None):
    first = start is None
    _, near, _, across, channels = x.shape
    pairs = near + 2
    span = pairs - 1
    groups, width = conv_weight.shape[2:4]
    count = near * (across // 2)
    out = jax.ShapeDtypeStruct((count, channels), jnp.float32)
    anywhere = pl.BlockSpec(memory_space=pltpu.HBM)
    vmem = pl.BlockSpec(memory_space=pltpu.VMEM)
    args = [x, up, down, conv_weight, point_weight, depth_weight] + ([] if first else [start])
    planes = (0, 2) if first else (1,)
    return pl.pallas_call(
        lambda *refs: block_kernel(frame, planes, first, refs),
        out_shape=[jax.ShapeDtypeStruct(out.shape, jnp.bfloat16), out] if first else out,
        in_specs=[anywhere, vmem, vmem, anywhere, anywhere] + [vmem] * (1 if first else 2),
        out_specs=[vmem, vmem] if first else vmem,
        scratch_shapes=[
            pltpu.VMEM((pairs, 2, across, channels), jnp.bfloat16),
            pltpu.VMEM((pairs, 2, across, channels), jnp.bfloat16),
            pltpu.VMEM((pairs, 2, across, channels), jnp.bfloat16),
            pltpu.VMEM(conv_weight.shape, jnp.bfloat16),
            pltpu.VMEM(point_weight.shape, jnp.bfloat16),
            pltpu.VMEM((span, 2, across, channels), jnp.float32),
            pltpu.VMEM((span, 2, across, channels), jnp.bfloat16),
            pltpu.VMEM((groups, 2 * span, across + 8, width), jnp.float32),
            pltpu.SemaphoreType.DMA((4,)),
            pltpu.SemaphoreType.DMA((groups,)),
        ],
        compiler_params=pltpu.CompilerParams(vmem_limit_bytes=60 << 20),
        name="block_last" if first else "block_first",
    )(*args)


HBM = pl.BlockSpec(memory_space=pltpu.HBM)
VMEM = pl.BlockSpec(memory_space=pltpu.VMEM)
SMEM = pl.BlockSpec(memory_space=pltpu.SMEM)


def run_copies(copies):
    for copy in copies:
        copy.start()
    for copy in copies:
        copy.wait()


def cut_kernel(weight_ref, x_ref, *refs):
    _, _, inner, cores = axes_of()
    g, _, y, c = place_of()
    head, tail, pieces, sem = refs[0], refs[1], refs[2:-1], refs[-1]
    block = pieces[0].shape[1]
    near = x_ref.shape[1]
    copies = [
        pltpu.make_async_copy(x_ref.at[:, 0], head, sem.at[len(pieces)]),
        pltpu.make_async_copy(x_ref.at[:, near - 1], tail, sem.at[len(pieces) + 1]),
    ]
    for n, (dy, dc) in enumerate(itertools.product(range(inner), range(cores))):
        to = (g * inner + lax.rem(y + dy, inner)) * cores + lax.rem(c + dc, cores)
        lanes = pl.ds(pl.multiple_of(to * block, 128), block)
        copies.append(pltpu.make_async_copy(weight_ref.at[:, lanes], pieces[n], sem.at[n]))
    run_copies(copies)


def join_kernel(*refs):
    _, _, inner, cores = axes_of()
    _, _, y, c = place_of()
    pieces, level_ref = refs[:-1], refs[-1]
    depth = pieces[0].shape[0]
    for n, (dy, dc) in enumerate(itertools.product(range(inner), range(cores))):
        source = lax.rem(y + inner - dy, inner) * cores + lax.rem(c + cores - dc, cores)
        level_ref[pl.ds(pl.multiple_of(source * depth, 8), depth), :] = pieces[n][...]


def cut(proj_weight, paired):
    groups, _, inner, cores = axes_of()
    g, _, y, c = place_of()
    depth, width = proj_weight.shape
    block = width // (groups * inner * cores)
    steps = list(itertools.product(range(inner), range(cores)))
    if depth % 8 or block % 128:
        to = [(g * inner + (y + dy) % inner) * cores + (c + dc) % cores for dy, dc in steps]
        pieces = [lax.dynamic_slice_in_dim(proj_weight, t * block, block, axis=1) for t in to]
        return paired[:, 0], paired[:, -1], pieces
    edge = jax.ShapeDtypeStruct(paired.shape[:1] + paired.shape[2:], paired.dtype)
    head, tail, *pieces = pl.pallas_call(
        cut_kernel,
        out_shape=[edge, edge] + [jax.ShapeDtypeStruct((depth, block), proj_weight.dtype)] * len(steps),
        in_specs=[HBM, HBM],
        out_specs=[VMEM] * (len(steps) + 2),
        scratch_shapes=[pltpu.SemaphoreType.DMA((len(steps) + 2,))],
        compiler_params=pltpu.CompilerParams(vmem_limit_bytes=60 << 20),
        name="cut",
    )(proj_weight, paired)
    return head, tail, pieces


def walk(outer):
    pairs = [n ^ 1 if n ^ 1 < outer else n for n in range(outer)]
    links = [((n - 1) ^ 1) + 1 if 0 < n and ((n - 1) ^ 1) + 1 < outer else n for n in range(outer)]
    own = list(range(outer))
    moves, pieces = [], [own]
    last = {"pairs": 0, "links": 0}
    missing = [set(own) - {n} for n in own]
    stage = 1
    while any(missing):
        done = dict(last)
        for name, other, perm in (("pairs", "links", pairs), ("links", "pairs", links)):
            source = done[other] if stage > 1 else 0
            if source is None:
                continue
            got = [pieces[source][perm[n]] for n in own]
            if not any(got[n] in missing[n] for n in own):
                last[name] = None
                continue
            moves.append((stage, source, perm))
            pieces.append(got)
            last[name] = len(pieces) - 1
            for n in own:
                missing[n].discard(got[n])
        stage += 1
    return moves, pieces


def slot_of(pieces, n, z):
    outer = len(pieces[0])
    slot = 0
    for here in range(outer):
        fresh = all(pieces[m][here] != pieces[n][here] for m in range(n))
        slot = jnp.where(z == here, pieces[n][here] if fresh else -1, slot)
    return slot


def fast(block, outer, peers, count):
    share = count // (outer * peers)
    return share % 8 == 0 and lax.axis_size("rows") * share % 16 == 0 and block % (256 * CHUNKS) == 0


def spread_weight(pieces, count):
    _, outer, inner, cores = axes_of()
    _, _, y, c = place_of()
    depth, block = pieces[0].shape
    steps = list(itertools.product(range(inner), range(cores)))
    pieces = [shifted(piece, (0, 0, dy, dc)) for piece, (dy, dc) in zip(pieces, steps)]
    rows = len(steps) * depth
    if depth % 8 == 0 and block % 128 == 0:
        level = pl.pallas_call(
            join_kernel,
            out_shape=jax.ShapeDtypeStruct((rows, block), pieces[0].dtype),
            in_specs=[VMEM] * len(steps),
            out_specs=VMEM,
            compiler_params=pltpu.CompilerParams(vmem_limit_bytes=8 << 20),
            name="join",
        )(*pieces)
    else:
        level = jnp.zeros((rows, block), pieces[0].dtype)
        for piece, (dy, dc) in zip(pieces, steps):
            at = ((y - dy) % inner) * cores + (c - dc) % cores
            level = lax.dynamic_update_slice_in_dim(level, piece, at * depth, axis=0)
    fits = fast(block, outer, len(steps), count)
    chunks = CHUNKS if fits else 1
    moves = walk(outer)[0]
    levels = [[level] for _ in range(chunks)]
    for stage, source, perm in moves:
        whole = [(n * inner + m, perm[n] * inner + m) for n in range(outer) for m in range(inner)]
        width = block if stage == 1 else block // chunks
        for h in range(chunks if stage > 1 else 1):
            value = levels[h][source]
            if value.shape[1] != width:
                value = value[:, h * width : (h + 1) * width]
            value = lax.ppermute(value, "tm", whole)
            for to in range(chunks) if stage == 1 else [h]:
                levels[to].append(value)
    return levels


def project_kernel(chunk, outer, inner, cores, *refs):
    peers = inner * cores
    held = walk(outer)[1]
    x_refs, refs = refs[:peers], refs[peers:]
    w_refs, refs = refs[: len(held)], refs[len(held) :]
    out_refs, (xs, ws, product, x_sem, w_sem) = refs[:peers], refs[peers:]
    _, z, y, c = place_of()
    count = x_refs[0].shape[0]
    rows, block = ws.shape[0] // outer, ws.shape[1]
    share = count // (outer * peers)
    w_refs = [
        w if w.shape[1] == block else w.at[:, pl.ds(chunk * block, block)] for w in w_refs
    ]
    for n, x_ref in enumerate(x_refs):
        pltpu.make_async_copy(x_ref, xs.at[pl.ds(n * count, count)], x_sem.at[n]).start()
    for n, w_ref in enumerate(w_refs):
        slot = slot_of(held, n, z)

        @pl.when(slot >= 0)
        def _():
            into = ws.at[pl.ds(pl.multiple_of(slot * rows, 16), rows)]
            pltpu.make_async_copy(w_ref, into, w_sem.at[n]).start()

    for n, x_ref in enumerate(x_refs):
        pltpu.make_async_copy(x_ref, xs.at[pl.ds(n * count, count)], x_sem.at[n]).wait()
    for n, w_ref in enumerate(w_refs):
        slot = slot_of(held, n, z)

        @pl.when(slot >= 0)
        def _():
            into = ws.at[pl.ds(pl.multiple_of(slot * rows, 16), rows)]
            pltpu.make_async_copy(w_ref, into, w_sem.at[n]).wait()

    def multiply(n, carry):
        lanes = pl.ds(pl.multiple_of(n * 256, 256), 256)
        out = jnp.dot(xs[...], ws[:, lanes], preferred_element_type=jnp.float32)
        product[:, :, :, :, lanes] = out.reshape(peers, outer, peers, share, 256)
        return carry

    lax.fori_loop(0, block // 256, multiply, 0)
    for n, (ty, tc) in enumerate(itertools.product(range(inner), range(cores))):
        target = lax.rem(y + ty, inner) * cores + lax.rem(c + tc, cores)
        for dz, dy in itertools.product(range(outer), range(inner)):
            from_z, from_y = lax.rem(z + outer - dz, outer), lax.rem(y + inner - dy, inner)
            tiles = []
            for from_c in range(cores):
                dc = lax.rem(c + cores - from_c, cores)
                tiles.append(product[dy * cores + dc, dz, target])
            at = (from_z * inner + from_y) * cores * share
            tile = jnp.concatenate(tiles, axis=0).astype(jnp.bfloat16)
            out_refs[n][pl.ds(pl.multiple_of(at, cores * share), cores * share), :] = tile


def project_call(chunk, blocks, levels, outer, inner, cores):
    peers = inner * cores
    count, channels = blocks[0].shape
    rows, block = levels[0].shape
    block //= CHUNKS
    share = count // (outer * peers)
    return pl.pallas_call(
        lambda *refs: project_kernel(chunk, outer, inner, cores, *refs),
        out_shape=[jax.ShapeDtypeStruct((count, block), jnp.bfloat16)] * peers,
        in_specs=[HBM] * (peers + len(levels)),
        out_specs=[VMEM] * peers,
        scratch_shapes=[
            pltpu.VMEM((peers * count, channels), jnp.bfloat16),
            pltpu.VMEM((outer * rows, block), jnp.bfloat16),
            pltpu.VMEM((peers, outer, peers, share, block), jnp.float32),
            pltpu.SemaphoreType.DMA((peers,)),
            pltpu.SemaphoreType.DMA((len(levels),)),
        ],
        compiler_params=pltpu.CompilerParams(vmem_limit_bytes=32 << 20),
        name="project",
    )(*blocks, *levels)


def project_plain(chunk, blocks, levels, outer, inner, cores):
    _, z, y, c = place_of()
    peers = inner * cores
    count, channels = blocks[0].shape
    block = levels[0].shape[1]
    share = count // (outer * peers)
    held = walk(outer)[1]
    whole = jnp.zeros((outer,) + levels[0].shape, levels[0].dtype)
    for n, level in enumerate(levels):
        slot = slot_of(held, n, z)
        at = jnp.maximum(slot, 0)
        kept = lax.dynamic_index_in_dim(whole, at, 0, False)
        level = jnp.where(slot >= 0, level, kept)
        whole = lax.dynamic_update_slice_in_dim(whole, level[None], at, axis=0)
    every = jnp.zeros((inner, cores, outer, peers, share, channels), jnp.bfloat16)
    for n, (dy, dc) in enumerate(itertools.product(range(inner), range(cores))):
        piece = blocks[n].reshape(outer, peers, share, channels)
        piece = jnp.roll(piece[(-jnp.arange(outer)) % outer], z, axis=0)
        every = lax.dynamic_update_slice(
            every, piece[None, None], ((y - dy) % inner, (c - dc) % cores, 0, 0, 0, 0)
        )
    every = jnp.transpose(every, (3, 2, 0, 1, 4, 5)).reshape(-1, channels)
    product = jnp.dot(every, whole.reshape(-1, block), preferred_element_type=jnp.float32)
    product = product.astype(jnp.bfloat16).reshape(peers, count, block)
    return [
        lax.dynamic_index_in_dim(product, ((y + ty) % inner) * cores + (c + tc) % cores, 0, False)
        for ty, tc in itertools.product(range(inner), range(cores))
    ]


def collect_kernel(*refs):
    groups, _, inner, cores = axes_of()
    g, _, y, c = place_of()
    pieces, out_ref, sem = refs[:-2], refs[-2], refs[-1]
    block = pieces[0].shape[1]
    chunks = len(pieces) // (groups * inner * cores)
    copies = []
    where = itertools.product(range(groups), range(inner), range(cores), range(chunks))
    for n, (dg, dy, dc, h) in enumerate(where):
        source = lax.rem(g + groups - dg, groups) * inner + lax.rem(y + inner - dy, inner)
        source = source * cores + lax.rem(c + cores - dc, cores)
        lanes = pl.ds(pl.multiple_of((source * chunks + h) * block, 128), block)
        copies.append(pltpu.make_async_copy(pieces[n], out_ref.at[:, lanes], sem.at[n]))
    run_copies(copies)


def deliver(placed, levels):
    groups, outer, inner, cores = axes_of()
    g, _, y, c = place_of()
    count, _ = placed.shape
    block = levels[0][0].shape[1]
    part = count // outer
    mine = [shifted(placed[dz * part : (dz + 1) * part], (0, dz, 0, 0)) for dz in range(outer)]
    mine = jnp.concatenate(mine, axis=0)
    chips = {}
    for dg, dy in itertools.product(reversed(range(groups)), reversed(range(inner))):
        chips[dg, dy] = shifted(mine, (dg, 0, dy, 0))
    blocks = {}
    for dg, dy, dc in itertools.product(range(groups), range(inner), range(cores)):
        blocks[dg, dy, dc] = shifted(chips[dg, dy], (0, 0, 0, dc))
    fits = fast(block, outer, inner * cores, count)
    call = project_call if fits else project_plain
    steps = list(itertools.product(range(inner), range(cores)))
    arrived = {}
    for h, held in enumerate(levels):
        for dg in reversed(range(groups)):
            group = [blocks[dg, dy, dc] for dy, dc in steps]
            pieces = call(h, group, held, outer, inner, cores)
            for (dy, dc), piece in zip(steps, pieces):
                arrived[dg, dy, dc, h] = shifted(piece, (dg, 0, dy, dc))
    if fits:
        pieces = [piece for _, piece in sorted(arrived.items())]
        return pl.pallas_call(
            collect_kernel,
            out_shape=jax.ShapeDtypeStruct((count, len(pieces) // len(levels) * block), jnp.bfloat16),
            in_specs=[VMEM] * len(pieces),
            out_specs=HBM,
            scratch_shapes=[pltpu.SemaphoreType.DMA((len(pieces),))],
            compiler_params=pltpu.CompilerParams(vmem_limit_bytes=8 << 20),
            name="collect",
        )(*pieces)
    out = jnp.zeros((count, groups * inner * cores * block), jnp.bfloat16)
    for (dg, dy, dc, _), piece in sorted(arrived.items()):
        source = (((g - dg) % groups) * inner + (y - dy) % inner) * cores + (c - dc) % cores
        out = lax.dynamic_update_slice_in_dim(out, piece, source * block, axis=1)
    return out


def place_kernel(spans, sum_ref, rim_ref, target_ref, placed_ref):
    count = sum_ref.shape[0]
    rim = rim_ref[...].astype(jnp.float32)
    row = lax.broadcasted_iota(jnp.int32, rim.shape, 0)
    rim = jnp.where((row < count // spans) & (lax.axis_index("tm") == 0), 0.0, rim)
    tokens = silu(sum_ref[...] + rim).astype(jnp.bfloat16)
    slot = lax.broadcasted_iota(jnp.int32, (count, count), 0)
    selector = jnp.where(slot == target_ref[...], 1.0, 0.0).astype(jnp.bfloat16)
    placed = jnp.dot(selector, tokens, preferred_element_type=jnp.float32)
    placed_ref[...] = placed.astype(jnp.bfloat16)


def place_call(spans, total, rim, target):
    vmem = pl.BlockSpec(memory_space=pltpu.VMEM)
    return pl.pallas_call(
        lambda *refs: place_kernel(spans, *refs),
        out_shape=jax.ShapeDtypeStruct(total.shape, jnp.bfloat16),
        in_specs=[vmem] * 3,
        out_specs=vmem,
        compiler_params=pltpu.CompilerParams(vmem_limit_bytes=8 << 20),
        name="place",
    )(total, rim, target)


def slots(rank_order, count):
    _, outer, inner, cores = axes_of()
    _, z, _, _ = place_of()
    ranks = outer * inner * cores
    period = 2 * ranks
    share = count // ranks
    position = jnp.arange(count, dtype=jnp.int32)
    stripe = position % period
    folded = jnp.minimum(stripe, period - 1 - stripe)
    one_hot = folded[:, None] == jnp.arange(ranks, dtype=jnp.int32)[None, :]
    owner = jnp.sum(jnp.where(one_hot, rank_order[None, :], 0), axis=1)
    owner = (owner + (outer - z) * inner * cores) % ranks
    target = owner * share + (position // period) * 2 + (stripe >= ranks).astype(jnp.int32)
    return target.reshape(1, count)


def local(video_tokens, conv_weight, point_weight, depth_weight, proj_weight, rank_order):
    frames, height, across, channels = video_tokens.shape
    cores, along = lax.axis_size("rows"), lax.axis_size("tm")
    paired = video_tokens.reshape(frames, height // 2, 2, across, channels)
    head, tail, pieces = cut(proj_weight, paired)
    up = lax.ppermute(tail, "rows", [(i, (i + 1) % cores) for i in range(cores)])
    down = lax.ppermute(head, "rows", [((i + 1) % cores, i) for i in range(cores)])
    levels = spread_weight(pieces, frames // 2 * (height // 2) * (across // 2))
    shared = (paired, up, down, conv_weight, point_weight, depth_weight)
    sums, rims = [], []
    for o in reversed(range(frames // 2)):
        sent, kept = block_call(2 * o + 1, *shared)
        rims.insert(0, sent)
        sums.insert(0, block_call(2 * o, *shared, kept))
    rim = lax.ppermute(rims[-1], "tm", [(i, (i + 1) % along) for i in range(along)])
    if frames > 2:
        rim = jnp.concatenate([rim] + rims[:-1], axis=0)
    total = sums[0] if len(sums) == 1 else jnp.concatenate(sums, axis=0)
    placed = place_call(frames // 2, total, rim, slots(rank_order, total.shape[0]))
    return deliver(placed, levels)


def solution(mesh):
    return jax.shard_map(
        local,
        mesh=mesh,
        in_specs=(
            P(("groups", "tm"), "rows", None, None),
            P(),
            P(),
            P(),
            P(("tm", "rows"), None),
            P("groups"),
        ),
        out_specs=P(("groups", "tm", "rows"), None),
        check_vma=False,
    )
```

```python
import itertools
import math

import jax
import jax.numpy as jnp
from jax import lax
from jax.experimental import pallas as pl
from jax.experimental.pallas import tpu as pltpu
from jax.sharding import PartitionSpec as P

AXES = ("groups", "tm", "rows")
SPREAD = 2
CHUNKS = 2


def axes_of():
    groups, count, cores = (lax.axis_size(a) for a in AXES)
    inner = math.gcd(count, SPREAD)
    return groups, count // inner, inner, cores


def place_of():
    _, _, inner, _ = axes_of()
    along = lax.axis_index("tm")
    return lax.axis_index("groups"), along // inner, along % inner, lax.axis_index("rows")


def shifted(value, steps):
    sizes = axes_of()
    if not any(steps):
        return value
    pairs = []
    for source, here in enumerate(itertools.product(*(range(n) for n in sizes))):
        there = [(a + b) % n for a, b, n in zip(here, steps, sizes)]
        target = 0
        for a, n in zip(there, sizes):
            target = target * n + a
        pairs.append((source, target))
    return lax.ppermute(value, AXES, pairs)


def silu(values):
    half = 0.5 * values
    return half + half * jnp.tanh(half)


def normal(values):
    scale = 1.0 / values.shape[-1]
    centred = values - jnp.sum(values, axis=-1, keepdims=True) * scale
    spread = jnp.sum(centred * centred, axis=-1, keepdims=True) * scale
    return centred * lax.rsqrt(spread + 1e-05)


def block_kernel(frame, planes, first, refs):
    if first:
        (x_hbm, up_ref, down_ref, conv_hbm, point_hbm, depth_ref, sent_ref, kept_ref,
         xin, xl, xr, conv_v, point_v, wide, act, rim, sems, conv_sems) = refs
        start_ref, out_refs = None, (sent_ref, kept_ref)
    else:
        (x_hbm, up_ref, down_ref, conv_hbm, point_hbm, depth_ref, start_ref, kept_ref,
         xin, xl, xr, conv_v, point_v, wide, act, rim, sems, conv_sems) = refs
        out_refs = (kept_ref,)
    pairs, _, across, channels = xin.shape
    width = conv_v.shape[-1]
    groups = channels // width
    copies = [
        pltpu.make_async_copy(x_hbm.at[frame], xin.at[pl.ds(1, pairs - 2)], sems.at[0]),
    ]

    def conv_copy(g):
        return pltpu.make_async_copy(conv_hbm.at[:, :, g], conv_v.at[:, :, g], conv_sems.at[g])

    point_copy = pltpu.make_async_copy(point_hbm, point_v, sems.at[3])
    for copy in copies + [conv_copy(g) for g in range(groups)] + [point_copy]:
        copy.start()
    for copy in copies:
        copy.wait()
    core, cores = lax.axis_index("rows"), lax.axis_size("rows")
    blank = jnp.zeros(xin.shape[1:], jnp.bfloat16)
    xin[0] = jnp.where(core == 0, blank, up_ref[frame])
    xin[pairs - 1] = jnp.where(core == cores - 1, blank, down_ref[frame])
    column = lax.broadcasted_iota(jnp.int32, (across, channels), 0)

    def shift(i, carry):
        k, p = i // 2, i % 2
        row = xin[k, p].astype(jnp.float32)
        left = jnp.where(column == 0, 0.0, pltpu.roll(row, 1, 0))
        right = jnp.where(column == across - 1, 0.0, pltpu.roll(row, across - 1, 0))
        xl[k, p] = left.astype(jnp.bfloat16)
        xr[k, p] = right.astype(jnp.bfloat16)
        return carry

    lax.fori_loop(0, 2 * pairs, shift, 0)

    span = pairs - 1
    order = []
    for half in (0, 2):
        order += [(half, 0), (half, 1), (half + 1, 0), (half + 1, 1), (half, 2), (half + 1, 2)]
    sources = (xl, xin, xr)
    zero = jnp.zeros((width, width), jnp.bfloat16)

    def convolve(g, carry):
        lanes = pl.ds(pl.multiple_of(g * width, width), width)
        conv_copy(g).wait()
        left_side, right_side = [], []
        for a, b in order:
            piece = sources[b][pl.ds(a // 2, span), a % 2, :, lanes]
            left_side.append(piece.reshape(span * across, width))
            taps = [conv_v[a - j, b, g] if 0 <= a - j < 3 else zero for j in range(2)]
            right_side.append(jnp.concatenate(taps, axis=1))
        out = jnp.dot(
            jnp.concatenate(left_side, axis=1),
            jnp.concatenate(right_side, axis=0),
            preferred_element_type=jnp.float32,
        )
        for j in range(2):
            wide[:, j, :, lanes] = out[:, j * width : (j + 1) * width].reshape(span, across, width)
        return carry

    lax.fori_loop(0, groups, convolve, 0)

    def activate(i, carry):
        for p in range(2):
            for h in range(0, across, 16):
                act[i, p, pl.ds(h, 16)] = silu(normal(wide[i, p, pl.ds(h, 16)])).astype(jnp.bfloat16)
        return carry

    lax.fori_loop(0, span, activate, 0, unroll=3)
    point_copy.wait()
    step = 2 * width

    def mix(at, lanes):
        product = jnp.dot(
            act[...].reshape(2 * span * across, channels),
            point_v[:, lanes],
            preferred_element_type=jnp.float32,
        )
        wide[:, :, :, lanes] = product.reshape(span, 2, across, product.shape[1])
        return at

    lax.fori_loop(0, channels // step, lambda n, t: mix(t, pl.ds(pl.multiple_of(n * step, step), step)), 0, unroll=True)
    if channels % step:
        mix(0, pl.ds(channels // step * step, channels % step))

    margin = rim.shape[2] - across
    keep = jnp.where(core == 0, 0.0, 1.0)

    def finish(i, carry):
        for p in range(2):
            for h in range(0, across, 16):
                value = xin[i + p, 1 - p, pl.ds(h, 16)].astype(jnp.float32)
                value = silu(value + normal(wide[i, p, pl.ds(h, 16)]))
                if p == 0:
                    value = jnp.where(i == 0, value * keep, value)
                for g in range(groups):
                    rim[g, 2 * i + p, pl.ds(margin + h, 16), :] = value[:, g * width : (g + 1) * width]
            for g in range(groups):
                rim[g, 2 * i + p, pl.ds(0, margin), :] = jnp.zeros((margin, width), jnp.float32)
        return carry

    lax.fori_loop(0, span, finish, 0, unroll=3)

    half = across // 2

    def sample_group(g, outer):
        lanes = pl.ds(pl.multiple_of(g * width, width), width)
        weights = [
            [
                jnp.broadcast_to(
                    depth_ref[plane, tap // 3, pl.ds(tap % 3, 1), lanes].astype(jnp.float32), (8, width)
                )
                for tap in range(9)
            ]
            for plane in planes
        ]

        def sample(p, carry):
            for t in range(half // 8):
                where = pl.ds(pl.multiple_of(p * half + 8 * t, 8), 8)
                totals = [None] * len(planes)
                if start_ref is not None:
                    totals[0] = start_ref[where, lanes]
                for b in range(3):
                    for e in range(3):
                        value = rim[g, 2 * p + b, pl.ds(margin - 1 + e + 16 * t, 8, 2), :]
                        for n in range(len(planes)):
                            term = weights[n][3 * b + e] * value
                            totals[n] = term if totals[n] is None else totals[n] + term
                for ref, total in zip(out_refs, totals):
                    ref[where, lanes] = total.astype(ref.dtype)
            return carry

        lax.fori_loop(0, span - 1, sample, 0, unroll=2)
        return outer

    lax.fori_loop(0, groups, sample_group, 0)


def block_call(frame, x, up, down, conv_weight, point_weight, depth_weight, start=None):
    first = start is None
    _, near, _, across, channels = x.shape
    pairs = near + 2
    span = pairs - 1
    groups, width = conv_weight.shape[2:4]
    count = near * (across // 2)
    out = jax.ShapeDtypeStruct((count, channels), jnp.float32)
    anywhere = pl.BlockSpec(memory_space=pltpu.HBM)
    vmem = pl.BlockSpec(memory_space=pltpu.VMEM)
    args = [x, up, down, conv_weight, point_weight, depth_weight] + ([] if first else [start])
    planes = (0, 2) if first else (1,)
    return pl.pallas_call(
        lambda *refs: block_kernel(frame, planes, first, refs),
        out_shape=[jax.ShapeDtypeStruct(out.shape, jnp.bfloat16), out] if first else out,
        in_specs=[anywhere, vmem, vmem, anywhere, anywhere] + [vmem] * (1 if first else 2),
        out_specs=[vmem, vmem] if first else vmem,
        scratch_shapes=[
            pltpu.VMEM((pairs, 2, across, channels), jnp.bfloat16),
            pltpu.VMEM((pairs, 2, across, channels), jnp.bfloat16),
            pltpu.VMEM((pairs, 2, across, channels), jnp.bfloat16),
            pltpu.VMEM(conv_weight.shape, jnp.bfloat16),
            pltpu.VMEM(point_weight.shape, jnp.bfloat16),
            pltpu.VMEM((span, 2, across, channels), jnp.float32),
            pltpu.VMEM((span, 2, across, channels), jnp.bfloat16),
            pltpu.VMEM((groups, 2 * span, across + 8, width), jnp.float32),
            pltpu.SemaphoreType.DMA((4,)),
            pltpu.SemaphoreType.DMA((groups,)),
        ],
        compiler_params=pltpu.CompilerParams(vmem_limit_bytes=60 << 20),
        name="block_last" if first else "block_first",
    )(*args)


HBM = pl.BlockSpec(memory_space=pltpu.HBM)
VMEM = pl.BlockSpec(memory_space=pltpu.VMEM)
SMEM = pl.BlockSpec(memory_space=pltpu.SMEM)


def run_copies(copies):
    for copy in copies:
        copy.start()
    for copy in copies:
        copy.wait()


def cut_kernel(weight_ref, x_ref, *refs):
    _, _, inner, cores = axes_of()
    g, _, y, c = place_of()
    edges, pieces, sem = refs[: -1 - inner * cores], refs[-1 - inner * cores : -1], refs[-1]
    block = pieces[0].shape[1]
    near = x_ref.shape[1]
    rows = [jnp.where(c == 0, near - 1, 0)] if cores == 2 else [0, near - 1]
    copies = [
        pltpu.make_async_copy(x_ref.at[:, row], edge, sem.at[len(pieces) + n])
        for n, (row, edge) in enumerate(zip(rows, edges))
    ]
    for n, (dy, dc) in enumerate(itertools.product(range(inner), range(cores))):
        to = (g * inner + lax.rem(y + dy, inner)) * cores + lax.rem(c + dc, cores)
        lanes = pl.ds(pl.multiple_of(to * block, 128), block)
        copies.append(pltpu.make_async_copy(weight_ref.at[:, lanes], pieces[n], sem.at[n]))
    run_copies(copies)


def join_kernel(*refs):
    _, _, inner, cores = axes_of()
    _, _, y, c = place_of()
    pieces, level_ref = refs[:-1], refs[-1]
    depth = pieces[0].shape[0]
    for n, (dy, dc) in enumerate(itertools.product(range(inner), range(cores))):
        source = lax.rem(y + inner - dy, inner) * cores + lax.rem(c + cores - dc, cores)
        level_ref[pl.ds(pl.multiple_of(source * depth, 8), depth), :] = pieces[n][...]


def cut(proj_weight, paired):
    groups, _, inner, cores = axes_of()
    g, _, y, c = place_of()
    depth, width = proj_weight.shape
    block = width // (groups * inner * cores)
    steps = list(itertools.product(range(inner), range(cores)))
    if depth % 8 or block % 128:
        to = [(g * inner + (y + dy) % inner) * cores + (c + dc) % cores for dy, dc in steps]
        pieces = [lax.dynamic_slice_in_dim(proj_weight, t * block, block, axis=1) for t in to]
        if cores == 2:
            return [jnp.where(c == 0, paired[:, -1], paired[:, 0])], pieces
        return [paired[:, 0], paired[:, -1]], pieces
    edge = jax.ShapeDtypeStruct(paired.shape[:1] + paired.shape[2:], paired.dtype)
    sides = 1 if cores == 2 else 2
    found = pl.pallas_call(
        cut_kernel,
        out_shape=[edge] * sides + [jax.ShapeDtypeStruct((depth, block), proj_weight.dtype)] * len(steps),
        in_specs=[HBM, HBM],
        out_specs=[VMEM] * (len(steps) + sides),
        scratch_shapes=[pltpu.SemaphoreType.DMA((len(steps) + sides,))],
        compiler_params=pltpu.CompilerParams(vmem_limit_bytes=60 << 20),
        name="cut",
    )(proj_weight, paired)
    return found[:sides], found[sides:]


def walk(outer):
    pairs = [n ^ 1 if n ^ 1 < outer else n for n in range(outer)]
    links = [((n - 1) ^ 1) + 1 if 0 < n and ((n - 1) ^ 1) + 1 < outer else n for n in range(outer)]
    own = list(range(outer))
    moves, pieces = [], [own]
    last = {"pairs": 0, "links": 0}
    missing = [set(own) - {n} for n in own]
    stage = 1
    while any(missing):
        done = dict(last)
        for name, other, perm in (("pairs", "links", pairs), ("links", "pairs", links)):
            source = done[other] if stage > 1 else 0
            if source is None:
                continue
            got = [pieces[source][perm[n]] for n in own]
            if not any(got[n] in missing[n] for n in own):
                last[name] = None
                continue
            moves.append((stage, source, perm))
            pieces.append(got)
            last[name] = len(pieces) - 1
            for n in own:
                missing[n].discard(got[n])
        stage += 1
    return moves, pieces


def slot_of(pieces, n, z):
    outer = len(pieces[0])
    slot = 0
    for here in range(outer):
        fresh = all(pieces[m][here] != pieces[n][here] for m in range(n))
        slot = jnp.where(z == here, pieces[n][here] if fresh else -1, slot)
    return slot


def fast(block, outer, peers, count):
    share = count // (outer * peers)
    return share % 8 == 0 and lax.axis_size("rows") * share % 16 == 0 and block % (256 * CHUNKS) == 0


def spread_weight(pieces, count):
    _, outer, inner, cores = axes_of()
    _, _, y, c = place_of()
    depth, block = pieces[0].shape
    steps = list(itertools.product(range(inner), range(cores)))
    pieces = [shifted(piece, (0, 0, dy, dc)) for piece, (dy, dc) in zip(pieces, steps)]
    rows = len(steps) * depth
    if depth % 8 == 0 and block % 128 == 0:
        level = pl.pallas_call(
            join_kernel,
            out_shape=jax.ShapeDtypeStruct((rows, block), pieces[0].dtype),
            in_specs=[VMEM] * len(steps),
            out_specs=VMEM,
            compiler_params=pltpu.CompilerParams(vmem_limit_bytes=8 << 20),
            name="join",
        )(*pieces)
    else:
        level = jnp.zeros((rows, block), pieces[0].dtype)
        for piece, (dy, dc) in zip(pieces, steps):
            at = ((y - dy) % inner) * cores + (c - dc) % cores
            level = lax.dynamic_update_slice_in_dim(level, piece, at * depth, axis=0)
    fits = fast(block, outer, len(steps), count)
    chunks = CHUNKS if fits else 1
    moves = walk(outer)[0]
    levels = [[level] for _ in range(chunks)]
    for stage, source, perm in moves:
        whole = [(n * inner + m, perm[n] * inner + m) for n in range(outer) for m in range(inner)]
        width = block if stage == 1 else block // chunks
        for h in range(chunks if stage > 1 else 1):
            value = levels[h][source]
            if value.shape[1] != width:
                value = value[:, h * width : (h + 1) * width]
            value = lax.ppermute(value, "tm", whole)
            for to in range(chunks) if stage == 1 else [h]:
                levels[to].append(value)
    return levels


def project_kernel(chunk, outer, inner, cores, *refs):
    peers = inner * cores
    held = walk(outer)[1]
    x_refs, refs = refs[:peers], refs[peers:]
    w_refs, refs = refs[: len(held)], refs[len(held) :]
    out_refs, (xs, ws, product, x_sem, w_sem) = refs[:peers], refs[peers:]
    _, z, y, c = place_of()
    count = x_refs[0].shape[0]
    rows, block = ws.shape[0] // outer, ws.shape[1]
    share = count // (outer * peers)
    w_refs = [
        w if w.shape[1] == block else w.at[:, pl.ds(chunk * block, block)] for w in w_refs
    ]
    for n, x_ref in enumerate(x_refs):
        pltpu.make_async_copy(x_ref, xs.at[pl.ds(n * count, count)], x_sem.at[n]).start()
    for n, w_ref in enumerate(w_refs):
        slot = slot_of(held, n, z)

        @pl.when(slot >= 0)
        def _():
            into = ws.at[pl.ds(pl.multiple_of(slot * rows, 16), rows)]
            pltpu.make_async_copy(w_ref, into, w_sem.at[n]).start()

    for n, x_ref in enumerate(x_refs):
        pltpu.make_async_copy(x_ref, xs.at[pl.ds(n * count, count)], x_sem.at[n]).wait()
    for n, w_ref in enumerate(w_refs):
        slot = slot_of(held, n, z)

        @pl.when(slot >= 0)
        def _():
            into = ws.at[pl.ds(pl.multiple_of(slot * rows, 16), rows)]
            pltpu.make_async_copy(w_ref, into, w_sem.at[n]).wait()

    def multiply(n, carry):
        lanes = pl.ds(pl.multiple_of(n * 256, 256), 256)
        out = jnp.dot(xs[...], ws[:, lanes], preferred_element_type=jnp.float32)
        product[:, :, :, :, lanes] = out.reshape(peers, outer, peers, share, 256)
        return carry

    lax.fori_loop(0, block // 256, multiply, 0)
    for n, (ty, tc) in enumerate(itertools.product(range(inner), range(cores))):
        target = lax.rem(y + ty, inner) * cores + lax.rem(c + tc, cores)
        for dz, dy in itertools.product(range(outer), range(inner)):
            from_z, from_y = lax.rem(z + outer - dz, outer), lax.rem(y + inner - dy, inner)
            tiles = []
            for from_c in range(cores):
                dc = lax.rem(c + cores - from_c, cores)
                tiles.append(product[dy * cores + dc, dz, target])
            at = (from_z * inner + from_y) * cores * share
            tile = jnp.concatenate(tiles, axis=0).astype(jnp.bfloat16)
            out_refs[n][pl.ds(pl.multiple_of(at, cores * share), cores * share), :] = tile


def project_call(chunk, blocks, levels, outer, inner, cores):
    peers = inner * cores
    count, channels = blocks[0].shape
    rows, block = levels[0].shape
    block //= CHUNKS
    share = count // (outer * peers)
    return pl.pallas_call(
        lambda *refs: project_kernel(chunk, outer, inner, cores, *refs),
        out_shape=[jax.ShapeDtypeStruct((count, block), jnp.bfloat16)] * peers,
        in_specs=[HBM] * (peers + len(levels)),
        out_specs=[VMEM] * peers,
        scratch_shapes=[
            pltpu.VMEM((peers * count, channels), jnp.bfloat16),
            pltpu.VMEM((outer * rows, block), jnp.bfloat16),
            pltpu.VMEM((peers, outer, peers, share, block), jnp.float32),
            pltpu.SemaphoreType.DMA((peers,)),
            pltpu.SemaphoreType.DMA((len(levels),)),
        ],
        compiler_params=pltpu.CompilerParams(vmem_limit_bytes=32 << 20),
        name="project",
    )(*blocks, *levels)


def project_plain(chunk, blocks, levels, outer, inner, cores):
    _, z, y, c = place_of()
    peers = inner * cores
    count, channels = blocks[0].shape
    block = levels[0].shape[1]
    share = count // (outer * peers)
    held = walk(outer)[1]
    whole = jnp.zeros((outer,) + levels[0].shape, levels[0].dtype)
    for n, level in enumerate(levels):
        slot = slot_of(held, n, z)
        at = jnp.maximum(slot, 0)
        kept = lax.dynamic_index_in_dim(whole, at, 0, False)
        level = jnp.where(slot >= 0, level, kept)
        whole = lax.dynamic_update_slice_in_dim(whole, level[None], at, axis=0)
    every = jnp.zeros((inner, cores, outer, peers, share, channels), jnp.bfloat16)
    for n, (dy, dc) in enumerate(itertools.product(range(inner), range(cores))):
        piece = blocks[n].reshape(outer, peers, share, channels)
        piece = jnp.roll(piece[(-jnp.arange(outer)) % outer], z, axis=0)
        every = lax.dynamic_update_slice(
            every, piece[None, None], ((y - dy) % inner, (c - dc) % cores, 0, 0, 0, 0)
        )
    every = jnp.transpose(every, (3, 2, 0, 1, 4, 5)).reshape(-1, channels)
    product = jnp.dot(every, whole.reshape(-1, block), preferred_element_type=jnp.float32)
    product = product.astype(jnp.bfloat16).reshape(peers, count, block)
    return [
        lax.dynamic_index_in_dim(product, ((y + ty) % inner) * cores + (c + tc) % cores, 0, False)
        for ty, tc in itertools.product(range(inner), range(cores))
    ]


def collect_kernel(*refs):
    groups, _, inner, cores = axes_of()
    g, _, y, c = place_of()
    pieces, out_ref, sem = refs[:-2], refs[-2], refs[-1]
    block = pieces[0].shape[1]
    chunks = len(pieces) // (groups * inner * cores)
    copies = []
    where = itertools.product(range(groups), range(inner), range(cores), range(chunks))
    for n, (dg, dy, dc, h) in enumerate(where):
        source = lax.rem(g + groups - dg, groups) * inner + lax.rem(y + inner - dy, inner)
        source = source * cores + lax.rem(c + cores - dc, cores)
        lanes = pl.ds(pl.multiple_of((source * chunks + h) * block, 128), block)
        copies.append(pltpu.make_async_copy(pieces[n], out_ref.at[:, lanes], sem.at[n]))
    run_copies(copies)


def deliver(placed, levels):
    groups, outer, inner, cores = axes_of()
    g, _, y, c = place_of()
    count, _ = placed.shape
    block = levels[0][0].shape[1]
    part = count // outer
    mine = [shifted(placed[dz * part : (dz + 1) * part], (0, dz, 0, 0)) for dz in range(outer)]
    mine = jnp.concatenate(mine, axis=0)
    chips = {}
    for dg, dy in itertools.product(reversed(range(groups)), reversed(range(inner))):
        chips[dg, dy] = shifted(mine, (dg, 0, dy, 0))
    blocks = {}
    for dg, dy, dc in itertools.product(range(groups), range(inner), range(cores)):
        blocks[dg, dy, dc] = shifted(chips[dg, dy], (0, 0, 0, dc))
    fits = fast(block, outer, inner * cores, count)
    call = project_call if fits else project_plain
    steps = list(itertools.product(range(inner), range(cores)))
    arrived = {}
    for h, held in enumerate(levels):
        for dg in reversed(range(groups)):
            group = [blocks[dg, dy, dc] for dy, dc in steps]
            pieces = call(h, group, held, outer, inner, cores)
            for (dy, dc), piece in zip(steps, pieces):
                arrived[dg, dy, dc, h] = shifted(piece, (dg, 0, dy, dc))
    if fits:
        pieces = [piece for _, piece in sorted(arrived.items())]
        return pl.pallas_call(
            collect_kernel,
            out_shape=jax.ShapeDtypeStruct((count, len(pieces) // len(levels) * block), jnp.bfloat16),
            in_specs=[VMEM] * len(pieces),
            out_specs=HBM,
            scratch_shapes=[pltpu.SemaphoreType.DMA((len(pieces),))],
            compiler_params=pltpu.CompilerParams(vmem_limit_bytes=8 << 20),
            name="collect",
        )(*pieces)
    out = jnp.zeros((count, groups * inner * cores * block), jnp.bfloat16)
    for (dg, dy, dc, _), piece in sorted(arrived.items()):
        source = (((g - dg) % groups) * inner + (y - dy) % inner) * cores + (c - dc) % cores
        out = lax.dynamic_update_slice_in_dim(out, piece, source * block, axis=1)
    return out


def place_kernel(spans, sum_ref, rim_ref, target_ref, placed_ref):
    count = sum_ref.shape[0]
    rim = rim_ref[...].astype(jnp.float32)
    row = lax.broadcasted_iota(jnp.int32, rim.shape, 0)
    rim = jnp.where((row < count // spans) & (lax.axis_index("tm") == 0), 0.0, rim)
    tokens = silu(sum_ref[...] + rim).astype(jnp.bfloat16)
    slot = lax.broadcasted_iota(jnp.int32, (count, count), 0)
    selector = jnp.where(slot == target_ref[...], 1.0, 0.0).astype(jnp.bfloat16)
    placed = jnp.dot(selector, tokens, preferred_element_type=jnp.float32)
    placed_ref[...] = placed.astype(jnp.bfloat16)


def place_call(spans, total, rim, target):
    vmem = pl.BlockSpec(memory_space=pltpu.VMEM)
    return pl.pallas_call(
        lambda *refs: place_kernel(spans, *refs),
        out_shape=jax.ShapeDtypeStruct(total.shape, jnp.bfloat16),
        in_specs=[vmem] * 3,
        out_specs=vmem,
        compiler_params=pltpu.CompilerParams(vmem_limit_bytes=8 << 20),
        name="place",
    )(total, rim, target)


def slots(rank_order, count):
    _, outer, inner, cores = axes_of()
    _, z, _, _ = place_of()
    ranks = outer * inner * cores
    period = 2 * ranks
    share = count // ranks
    position = jnp.arange(count, dtype=jnp.int32)
    stripe = position % period
    folded = jnp.minimum(stripe, period - 1 - stripe)
    one_hot = folded[:, None] == jnp.arange(ranks, dtype=jnp.int32)[None, :]
    owner = jnp.sum(jnp.where(one_hot, rank_order[None, :], 0), axis=1)
    owner = (owner + (outer - z) * inner * cores) % ranks
    target = owner * share + (position // period) * 2 + (stripe >= ranks).astype(jnp.int32)
    return target.reshape(1, count)


def local(video_tokens, conv_weight, point_weight, depth_weight, proj_weight, rank_order):
    frames, height, across, channels = video_tokens.shape
    cores, along = lax.axis_size("rows"), lax.axis_size("tm")
    paired = video_tokens.reshape(frames, height // 2, 2, across, channels)
    edges, pieces = cut(proj_weight, paired)
    up = lax.ppermute(edges[-1], "rows", [(i, (i + 1) % cores) for i in range(cores)])
    down = up
    if len(edges) > 1:
        down = lax.ppermute(edges[0], "rows", [((i + 1) % cores, i) for i in range(cores)])
    levels = spread_weight(pieces, frames // 2 * (height // 2) * (across // 2))
    shared = (paired, up, down, conv_weight, point_weight, depth_weight)
    sums, rims = [], []
    for o in reversed(range(frames // 2)):
        sent, kept = block_call(2 * o + 1, *shared)
        rims.insert(0, sent)
        sums.insert(0, block_call(2 * o, *shared, kept))
    rim = lax.ppermute(rims[-1], "tm", [(i, (i + 1) % along) for i in range(along)])
    if frames > 2:
        rim = jnp.concatenate([rim] + rims[:-1], axis=0)
    total = sums[0] if len(sums) == 1 else jnp.concatenate(sums, axis=0)
    placed = place_call(frames // 2, total, rim, slots(rank_order, total.shape[0]))
    return deliver(placed, levels)


def solution(mesh):
    return jax.shard_map(
        local,
        mesh=mesh,
        in_specs=(
            P(("groups", "tm"), "rows", None, None),
            P(),
            P(),
            P(),
            P(("tm", "rows"), None),
            P("groups"),
        ),
        out_specs=P(("groups", "tm", "rows"), None),
        check_vma=False,
    )
```

```python
import itertools
import math

import jax
import jax.numpy as jnp
from jax import lax
from jax.experimental import pallas as pl
from jax.experimental.pallas import tpu as pltpu
from jax.sharding import PartitionSpec as P

AXES = ("groups", "tm", "rows")
SPREAD = 2
CHUNKS = 2


def axes_of():
    groups, count, cores = (lax.axis_size(a) for a in AXES)
    inner = math.gcd(count, SPREAD)
    return groups, count // inner, inner, cores


def place_of():
    _, _, inner, _ = axes_of()
    along = lax.axis_index("tm")
    return lax.axis_index("groups"), along // inner, along % inner, lax.axis_index("rows")


def shifted(value, steps):
    sizes = axes_of()
    if not any(steps):
        return value
    pairs = []
    for source, here in enumerate(itertools.product(*(range(n) for n in sizes))):
        there = [(a + b) % n for a, b, n in zip(here, steps, sizes)]
        target = 0
        for a, n in zip(there, sizes):
            target = target * n + a
        pairs.append((source, target))
    return lax.ppermute(value, AXES, pairs)


def silu(values):
    half = 0.5 * values
    return half + half * jnp.tanh(half)


def normal(values):
    scale = 1.0 / values.shape[-1]
    centred = values - jnp.sum(values, axis=-1, keepdims=True) * scale
    spread = jnp.sum(centred * centred, axis=-1, keepdims=True) * scale
    return centred * lax.rsqrt(spread + 1e-05)


def block_kernel(frame, planes, first, refs):
    if first:
        (x_hbm, up_ref, down_ref, conv_hbm, point_hbm, depth_ref, sent_ref, kept_ref,
         xin, xl, xr, conv_v, point_v, wide, act, rim, sems, conv_sems) = refs
        start_ref, out_refs = None, (sent_ref, kept_ref)
    else:
        (x_hbm, up_ref, down_ref, conv_hbm, point_hbm, depth_ref, start_ref, kept_ref,
         xin, xl, xr, conv_v, point_v, wide, act, rim, sems, conv_sems) = refs
        out_refs = (kept_ref,)
    pairs, _, across, channels = xin.shape
    width = conv_v.shape[-1]
    groups = channels // width
    copies = [
        pltpu.make_async_copy(x_hbm.at[frame], xin.at[pl.ds(1, pairs - 2)], sems.at[0]),
    ]

    def conv_copy(g):
        return pltpu.make_async_copy(conv_hbm.at[:, :, g], conv_v.at[:, :, g], conv_sems.at[g])

    point_copy = pltpu.make_async_copy(point_hbm, point_v, sems.at[3])
    for copy in copies + [conv_copy(g) for g in range(groups)] + [point_copy]:
        copy.start()
    for copy in copies:
        copy.wait()
    core, cores = lax.axis_index("rows"), lax.axis_size("rows")
    blank = jnp.zeros(xin.shape[1:], jnp.bfloat16)
    xin[0] = jnp.where(core == 0, blank, up_ref[frame])
    xin[pairs - 1] = jnp.where(core == cores - 1, blank, down_ref[frame])
    column = lax.broadcasted_iota(jnp.int32, (across, channels), 0)

    def shift(i, carry):
        k, p = i // 2, i % 2
        row = xin[k, p].astype(jnp.float32)
        left = jnp.where(column == 0, 0.0, pltpu.roll(row, 1, 0))
        right = jnp.where(column == across - 1, 0.0, pltpu.roll(row, across - 1, 0))
        xl[k, p] = left.astype(jnp.bfloat16)
        xr[k, p] = right.astype(jnp.bfloat16)
        return carry

    lax.fori_loop(0, 2 * pairs, shift, 0)

    span = pairs - 1
    order = []
    for half in (0, 2):
        order += [(half, 0), (half, 1), (half + 1, 0), (half + 1, 1), (half, 2), (half + 1, 2)]
    sources = (xl, xin, xr)
    zero = jnp.zeros((width, width), jnp.bfloat16)

    def convolve(g, carry):
        lanes = pl.ds(pl.multiple_of(g * width, width), width)
        conv_copy(g).wait()
        left_side, right_side = [], []
        for a, b in order:
            piece = sources[b][pl.ds(a // 2, span), a % 2, :, lanes]
            left_side.append(piece.reshape(span * across, width))
            taps = [conv_v[a - j, b, g] if 0 <= a - j < 3 else zero for j in range(2)]
            right_side.append(jnp.concatenate(taps, axis=1))
        out = jnp.dot(
            jnp.concatenate(left_side, axis=1),
            jnp.concatenate(right_side, axis=0),
            preferred_element_type=jnp.float32,
        )
        for j in range(2):
            wide[:, j, :, lanes] = out[:, j * width : (j + 1) * width].reshape(span, across, width)
        return carry

    lax.fori_loop(0, groups, convolve, 0)

    def activate(i, carry):
        for p in range(2):
            for h in range(0, across, 16):
                act[i, p, pl.ds(h, 16)] = silu(normal(wide[i, p, pl.ds(h, 16)])).astype(jnp.bfloat16)
        return carry

    lax.fori_loop(0, span, activate, 0, unroll=3)
    point_copy.wait()
    step = 2 * width

    def mix(at, lanes):
        product = jnp.dot(
            act[...].reshape(2 * span * across, channels),
            point_v[:, lanes],
            preferred_element_type=jnp.float32,
        )
        wide[:, :, :, lanes] = product.reshape(span, 2, across, product.shape[1])
        return at

    lax.fori_loop(0, channels // step, lambda n, t: mix(t, pl.ds(pl.multiple_of(n * step, step), step)), 0, unroll=True)
    if channels % step:
        mix(0, pl.ds(channels // step * step, channels % step))

    margin = rim.shape[2] - across
    keep = jnp.where(core == 0, 0.0, 1.0)

    def finish(i, carry):
        for p in range(2):
            for h in range(0, across, 16):
                value = xin[i + p, 1 - p, pl.ds(h, 16)].astype(jnp.float32)
                value = silu(value + normal(wide[i, p, pl.ds(h, 16)]))
                if p == 0:
                    value = jnp.where(i == 0, value * keep, value)
                for g in range(groups):
                    rim[g, 2 * i + p, pl.ds(margin + h, 16), :] = value[:, g * width : (g + 1) * width]
            for g in range(groups):
                rim[g, 2 * i + p, pl.ds(0, margin), :] = jnp.zeros((margin, width), jnp.float32)
        return carry

    lax.fori_loop(0, span, finish, 0, unroll=3)

    half = across // 2

    def sample_group(g, outer):
        lanes = pl.ds(pl.multiple_of(g * width, width), width)
        weights = [
            [
                jnp.broadcast_to(
                    depth_ref[plane, tap // 3, pl.ds(tap % 3, 1), lanes].astype(jnp.float32), (8, width)
                )
                for tap in range(9)
            ]
            for plane in planes
        ]

        def sample(p, carry):
            for t in range(half // 8):
                where = pl.ds(pl.multiple_of(p * half + 8 * t, 8), 8)
                totals = [None] * len(planes)
                if start_ref is not None:
                    totals[0] = start_ref[where, lanes]
                for b in range(3):
                    for e in range(3):
                        value = rim[g, 2 * p + b, pl.ds(margin - 1 + e + 16 * t, 8, 2), :]
                        for n in range(len(planes)):
                            term = weights[n][3 * b + e] * value
                            totals[n] = term if totals[n] is None else totals[n] + term
                for ref, total in zip(out_refs, totals):
                    ref[where, lanes] = total.astype(ref.dtype)
            return carry

        lax.fori_loop(0, span - 1, sample, 0, unroll=2)
        return outer

    lax.fori_loop(0, groups, sample_group, 0)


def block_call(frame, x, up, down, conv_weight, point_weight, depth_weight, start=None):
    first = start is None
    _, near, _, across, channels = x.shape
    pairs = near + 2
    span = pairs - 1
    groups, width = conv_weight.shape[2:4]
    count = near * (across // 2)
    out = jax.ShapeDtypeStruct((count, channels), jnp.float32)
    anywhere = pl.BlockSpec(memory_space=pltpu.HBM)
    vmem = pl.BlockSpec(memory_space=pltpu.VMEM)
    args = [x, up, down, conv_weight, point_weight, depth_weight] + ([] if first else [start])
    planes = (0, 2) if first else (1,)
    return pl.pallas_call(
        lambda *refs: block_kernel(frame, planes, first, refs),
        out_shape=[jax.ShapeDtypeStruct(out.shape, jnp.bfloat16), out] if first else out,
        in_specs=[anywhere, vmem, vmem, anywhere, anywhere] + [vmem] * (1 if first else 2),
        out_specs=[vmem, vmem] if first else vmem,
        scratch_shapes=[
            pltpu.VMEM((pairs, 2, across, channels), jnp.bfloat16),
            pltpu.VMEM((pairs, 2, across, channels), jnp.bfloat16),
            pltpu.VMEM((pairs, 2, across, channels), jnp.bfloat16),
            pltpu.VMEM(conv_weight.shape, jnp.bfloat16),
            pltpu.VMEM(point_weight.shape, jnp.bfloat16),
            pltpu.VMEM((span, 2, across, channels), jnp.float32),
            pltpu.VMEM((span, 2, across, channels), jnp.bfloat16),
            pltpu.VMEM((groups, 2 * span, across + 8, width), jnp.float32),
            pltpu.SemaphoreType.DMA((4,)),
            pltpu.SemaphoreType.DMA((groups,)),
        ],
        compiler_params=pltpu.CompilerParams(vmem_limit_bytes=60 << 20),
        name="block_last" if first else "block_first",
    )(*args)


HBM = pl.BlockSpec(memory_space=pltpu.HBM)
VMEM = pl.BlockSpec(memory_space=pltpu.VMEM)
SMEM = pl.BlockSpec(memory_space=pltpu.SMEM)


def run_copies(copies):
    for copy in copies:
        copy.start()
    for copy in copies:
        copy.wait()


def cut_kernel(weight_ref, x_ref, *refs):
    _, _, inner, cores = axes_of()
    g, _, y, c = place_of()
    edges, pieces, sem = refs[: -1 - inner * cores], refs[-1 - inner * cores : -1], refs[-1]
    block = pieces[0].shape[1]
    near = x_ref.shape[1]
    rows = [jnp.where(c == 0, near - 1, 0)] if cores == 2 else [0, near - 1]
    copies = [
        pltpu.make_async_copy(x_ref.at[:, row], edge, sem.at[len(pieces) + n])
        for n, (row, edge) in enumerate(zip(rows, edges))
    ]
    for n, (dy, dc) in enumerate(itertools.product(range(inner), range(cores))):
        to = (g * inner + lax.rem(y + dy, inner)) * cores + lax.rem(c + dc, cores)
        lanes = pl.ds(pl.multiple_of(to * block, 128), block)
        copies.append(pltpu.make_async_copy(weight_ref.at[:, lanes], pieces[n], sem.at[n]))
    run_copies(copies)


def join_kernel(*refs):
    _, _, inner, cores = axes_of()
    _, _, y, c = place_of()
    pieces, level_ref = refs[:-1], refs[-1]
    depth = pieces[0].shape[0]
    for n, (dy, dc) in enumerate(itertools.product(range(inner), range(cores))):
        source = lax.rem(y + inner - dy, inner) * cores + lax.rem(c + cores - dc, cores)
        level_ref[pl.ds(pl.multiple_of(source * depth, 8), depth), :] = pieces[n][...]


def cut(proj_weight, paired):
    groups, _, inner, cores = axes_of()
    g, _, y, c = place_of()
    depth, width = proj_weight.shape
    block = width // (groups * inner * cores)
    steps = list(itertools.product(range(inner), range(cores)))
    if depth % 8 or block % 128:
        to = [(g * inner + (y + dy) % inner) * cores + (c + dc) % cores for dy, dc in steps]
        pieces = [lax.dynamic_slice_in_dim(proj_weight, t * block, block, axis=1) for t in to]
        if cores == 2:
            return [jnp.where(c == 0, paired[:, -1], paired[:, 0])], pieces
        return [paired[:, 0], paired[:, -1]], pieces
    edge = jax.ShapeDtypeStruct(paired.shape[:1] + paired.shape[2:], paired.dtype)
    sides = 1 if cores == 2 else 2
    found = pl.pallas_call(
        cut_kernel,
        out_shape=[edge] * sides + [jax.ShapeDtypeStruct((depth, block), proj_weight.dtype)] * len(steps),
        in_specs=[HBM, HBM],
        out_specs=[VMEM] * (len(steps) + sides),
        scratch_shapes=[pltpu.SemaphoreType.DMA((len(steps) + sides,))],
        compiler_params=pltpu.CompilerParams(vmem_limit_bytes=60 << 20),
        name="cut",
    )(proj_weight, paired)
    return found[:sides], found[sides:]


def walk(outer):
    pairs = [n ^ 1 if n ^ 1 < outer else n for n in range(outer)]
    links = [((n - 1) ^ 1) + 1 if 0 < n and ((n - 1) ^ 1) + 1 < outer else n for n in range(outer)]
    own = list(range(outer))
    moves, pieces = [], [own]
    last = {"pairs": 0, "links": 0}
    missing = [set(own) - {n} for n in own]
    stage = 1
    while any(missing):
        done = dict(last)
        for name, other, perm in (("pairs", "links", pairs), ("links", "pairs", links)):
            source = done[other] if stage > 1 else 0
            if source is None:
                continue
            got = [pieces[source][perm[n]] for n in own]
            if not any(got[n] in missing[n] for n in own):
                last[name] = None
                continue
            moves.append((stage, source, perm))
            pieces.append(got)
            last[name] = len(pieces) - 1
            for n in own:
                missing[n].discard(got[n])
        stage += 1
    return moves, pieces


def slot_of(pieces, n, z):
    outer = len(pieces[0])
    slot = 0
    for here in range(outer):
        fresh = all(pieces[m][here] != pieces[n][here] for m in range(n))
        slot = jnp.where(z == here, pieces[n][here] if fresh else -1, slot)
    return slot


def fast(block, outer, peers, count):
    share = count // (outer * peers)
    return share % 8 == 0 and lax.axis_size("rows") * share % 16 == 0 and block % (256 * CHUNKS) == 0


def spread_weight(pieces, count):
    _, outer, inner, cores = axes_of()
    _, _, y, c = place_of()
    depth, block = pieces[0].shape
    steps = list(itertools.product(range(inner), range(cores)))
    pieces = [shifted(piece, (0, 0, dy, dc)) for piece, (dy, dc) in zip(pieces, steps)]
    rows = len(steps) * depth
    if depth % 8 == 0 and block % 128 == 0:
        level = pl.pallas_call(
            join_kernel,
            out_shape=jax.ShapeDtypeStruct((rows, block), pieces[0].dtype),
            in_specs=[VMEM] * len(steps),
            out_specs=VMEM,
            compiler_params=pltpu.CompilerParams(vmem_limit_bytes=8 << 20),
            name="join",
        )(*pieces)
    else:
        level = jnp.zeros((rows, block), pieces[0].dtype)
        for piece, (dy, dc) in zip(pieces, steps):
            at = ((y - dy) % inner) * cores + (c - dc) % cores
            level = lax.dynamic_update_slice_in_dim(level, piece, at * depth, axis=0)
    fits = fast(block, outer, len(steps), count)
    chunks = CHUNKS if fits else 1
    moves = walk(outer)[0]
    levels = [[level] for _ in range(chunks)]
    for stage, source, perm in moves:
        whole = [(n * inner + m, perm[n] * inner + m) for n in range(outer) for m in range(inner)]
        width = block if stage == 1 else block // chunks
        for h in range(chunks if stage > 1 else 1):
            value = levels[h][source]
            if value.shape[1] != width:
                value = value[:, h * width : (h + 1) * width]
            value = lax.ppermute(value, "tm", whole)
            for to in range(chunks) if stage == 1 else [h]:
                levels[to].append(value)
    return levels


def project_kernel(chunk, outer, inner, cores, *refs):
    peers = inner * cores
    held = walk(outer)[1]
    x_refs, refs = refs[:peers], refs[peers:]
    w_refs, refs = refs[: len(held)], refs[len(held) :]
    out_refs, (xs, ws, product, x_sem, w_sem) = refs[:peers], refs[peers:]
    _, z, y, c = place_of()
    count = x_refs[0].shape[0]
    rows, block = ws.shape[0] // outer, ws.shape[1]
    share = count // (outer * peers)
    w_refs = [
        w if w.shape[1] == block else w.at[:, pl.ds(chunk * block, block)] for w in w_refs
    ]
    for n, x_ref in enumerate(x_refs):
        pltpu.make_async_copy(x_ref, xs.at[pl.ds(n * count, count)], x_sem.at[n]).start()
    for n, w_ref in enumerate(w_refs):
        slot = slot_of(held, n, z)

        @pl.when(slot >= 0)
        def _():
            into = ws.at[pl.ds(pl.multiple_of(slot * rows, 16), rows)]
            pltpu.make_async_copy(w_ref, into, w_sem.at[n]).start()

    for n, x_ref in enumerate(x_refs):
        pltpu.make_async_copy(x_ref, xs.at[pl.ds(n * count, count)], x_sem.at[n]).wait()
    for n, w_ref in enumerate(w_refs):
        slot = slot_of(held, n, z)

        @pl.when(slot >= 0)
        def _():
            into = ws.at[pl.ds(pl.multiple_of(slot * rows, 16), rows)]
            pltpu.make_async_copy(w_ref, into, w_sem.at[n]).wait()

    def multiply(n, carry):
        lanes = pl.ds(pl.multiple_of(n * 256, 256), 256)
        out = jnp.dot(xs[...], ws[:, lanes], preferred_element_type=jnp.float32)
        product[:, :, :, :, lanes] = out.reshape(peers, outer, peers, share, 256)
        return carry

    lax.fori_loop(0, block // 256, multiply, 0)
    for n, (ty, tc) in enumerate(itertools.product(range(inner), range(cores))):
        target = lax.rem(y + ty, inner) * cores + lax.rem(c + tc, cores)
        for dz, dy in itertools.product(range(outer), range(inner)):
            from_z, from_y = lax.rem(z + outer - dz, outer), lax.rem(y + inner - dy, inner)
            tiles = []
            for from_c in range(cores):
                dc = lax.rem(c + cores - from_c, cores)
                tiles.append(product[dy * cores + dc, dz, target])
            at = (from_z * inner + from_y) * cores * share
            tile = jnp.concatenate(tiles, axis=0).astype(jnp.bfloat16)
            out_refs[n][pl.ds(pl.multiple_of(at, cores * share), cores * share), :] = tile


def project_call(chunk, blocks, levels, outer, inner, cores):
    peers = inner * cores
    count, channels = blocks[0].shape
    rows, block = levels[0].shape
    block //= CHUNKS
    share = count // (outer * peers)
    return pl.pallas_call(
        lambda *refs: project_kernel(chunk, outer, inner, cores, *refs),
        out_shape=[jax.ShapeDtypeStruct((count, block), jnp.bfloat16)] * peers,
        in_specs=[HBM] * (peers + len(levels)),
        out_specs=[VMEM] * peers,
        scratch_shapes=[
            pltpu.VMEM((peers * count, channels), jnp.bfloat16),
            pltpu.VMEM((outer * rows, block), jnp.bfloat16),
            pltpu.VMEM((peers, outer, peers, share, block), jnp.float32),
            pltpu.SemaphoreType.DMA((peers,)),
            pltpu.SemaphoreType.DMA((len(levels),)),
        ],
        compiler_params=pltpu.CompilerParams(vmem_limit_bytes=32 << 20),
        name="project",
    )(*blocks, *levels)


def project_plain(chunk, blocks, levels, outer, inner, cores):
    _, z, y, c = place_of()
    peers = inner * cores
    count, channels = blocks[0].shape
    block = levels[0].shape[1]
    share = count // (outer * peers)
    held = walk(outer)[1]
    whole = jnp.zeros((outer,) + levels[0].shape, levels[0].dtype)
    for n, level in enumerate(levels):
        slot = slot_of(held, n, z)
        at = jnp.maximum(slot, 0)
        kept = lax.dynamic_index_in_dim(whole, at, 0, False)
        level = jnp.where(slot >= 0, level, kept)
        whole = lax.dynamic_update_slice_in_dim(whole, level[None], at, axis=0)
    every = jnp.zeros((inner, cores, outer, peers, share, channels), jnp.bfloat16)
    for n, (dy, dc) in enumerate(itertools.product(range(inner), range(cores))):
        piece = blocks[n].reshape(outer, peers, share, channels)
        piece = jnp.roll(piece[(-jnp.arange(outer)) % outer], z, axis=0)
        every = lax.dynamic_update_slice(
            every, piece[None, None], ((y - dy) % inner, (c - dc) % cores, 0, 0, 0, 0)
        )
    every = jnp.transpose(every, (3, 2, 0, 1, 4, 5)).reshape(-1, channels)
    product = jnp.dot(every, whole.reshape(-1, block), preferred_element_type=jnp.float32)
    product = product.astype(jnp.bfloat16).reshape(peers, count, block)
    return [
        lax.dynamic_index_in_dim(product, ((y + ty) % inner) * cores + (c + tc) % cores, 0, False)
        for ty, tc in itertools.product(range(inner), range(cores))
    ]


def collect_kernel(h, chunks, *refs):
    groups, _, inner, cores = axes_of()
    g, _, y, c = place_of()
    pieces, out_ref, sem = refs[: groups * inner * cores], refs[-2], refs[-1]
    block = pieces[0].shape[1]
    copies = []
    where = itertools.product(range(groups), range(inner), range(cores))
    for n, (dg, dy, dc) in enumerate(where):
        source = lax.rem(g + groups - dg, groups) * inner + lax.rem(y + inner - dy, inner)
        source = source * cores + lax.rem(c + cores - dc, cores)
        lanes = pl.ds(pl.multiple_of((source * chunks + h) * block, 128), block)
        copies.append(pltpu.make_async_copy(pieces[n], out_ref.at[:, lanes], sem.at[n]))
    run_copies(copies)


def deliver(placed, levels):
    groups, outer, inner, cores = axes_of()
    g, _, y, c = place_of()
    count, _ = placed.shape
    block = levels[0][0].shape[1]
    part = count // outer
    mine = [shifted(placed[dz * part : (dz + 1) * part], (0, dz, 0, 0)) for dz in range(outer)]
    mine = jnp.concatenate(mine, axis=0)
    chips = {}
    for dg, dy in itertools.product(reversed(range(groups)), reversed(range(inner))):
        chips[dg, dy] = shifted(mine, (dg, 0, dy, 0))
    blocks = {}
    for dg, dy, dc in itertools.product(range(groups), range(inner), range(cores)):
        blocks[dg, dy, dc] = shifted(chips[dg, dy], (0, 0, 0, dc))
    fits = fast(block, outer, inner * cores, count)
    call = project_call if fits else project_plain
    steps = list(itertools.product(range(inner), range(cores)))
    arrived = {}
    for h, held in enumerate(levels):
        for dg in reversed(range(groups)):
            group = [blocks[dg, dy, dc] for dy, dc in steps]
            pieces = call(h, group, held, outer, inner, cores)
            for (dy, dc), piece in zip(steps, pieces):
                arrived[dg, dy, dc, h] = shifted(piece, (dg, 0, dy, dc))
    if fits:
        out = ()
        for h in range(len(levels)):
            pieces = [piece for key, piece in sorted(arrived.items()) if key[3] == h]
            out = (
                pl.pallas_call(
                    lambda *refs, h=h: collect_kernel(h, len(levels), *refs),
                    out_shape=jax.ShapeDtypeStruct((count, len(pieces) * block), jnp.bfloat16),
                    in_specs=[VMEM] * len(pieces) + [HBM] * len(out),
                    out_specs=HBM,
                    scratch_shapes=[pltpu.SemaphoreType.DMA((len(pieces),))],
                    input_output_aliases={len(pieces): 0} if out else {},
                    compiler_params=pltpu.CompilerParams(vmem_limit_bytes=8 << 20),
                    name="collect",
                )(*pieces, *out),
            )
        return out[0]
    out = jnp.zeros((count, groups * inner * cores * block), jnp.bfloat16)
    for (dg, dy, dc, _), piece in sorted(arrived.items()):
        source = (((g - dg) % groups) * inner + (y - dy) % inner) * cores + (c - dc) % cores
        out = lax.dynamic_update_slice_in_dim(out, piece, source * block, axis=1)
    return out


def place_kernel(spans, sum_ref, rim_ref, target_ref, placed_ref):
    count = sum_ref.shape[0]
    rim = rim_ref[...].astype(jnp.float32)
    row = lax.broadcasted_iota(jnp.int32, rim.shape, 0)
    rim = jnp.where((row < count // spans) & (lax.axis_index("tm") == 0), 0.0, rim)
    tokens = silu(sum_ref[...] + rim).astype(jnp.bfloat16)
    slot = lax.broadcasted_iota(jnp.int32, (count, count), 0)
    selector = jnp.where(slot == target_ref[...], 1.0, 0.0).astype(jnp.bfloat16)
    placed = jnp.dot(selector, tokens, preferred_element_type=jnp.float32)
    placed_ref[...] = placed.astype(jnp.bfloat16)


def place_call(spans, total, rim, target):
    vmem = pl.BlockSpec(memory_space=pltpu.VMEM)
    return pl.pallas_call(
        lambda *refs: place_kernel(spans, *refs),
        out_shape=jax.ShapeDtypeStruct(total.shape, jnp.bfloat16),
        in_specs=[vmem] * 3,
        out_specs=vmem,
        compiler_params=pltpu.CompilerParams(vmem_limit_bytes=8 << 20),
        name="place",
    )(total, rim, target)


def slots(rank_order, count):
    _, outer, inner, cores = axes_of()
    _, z, _, _ = place_of()
    ranks = outer * inner * cores
    period = 2 * ranks
    share = count // ranks
    position = jnp.arange(count, dtype=jnp.int32)
    stripe = position % period
    folded = jnp.minimum(stripe, period - 1 - stripe)
    one_hot = folded[:, None] == jnp.arange(ranks, dtype=jnp.int32)[None, :]
    owner = jnp.sum(jnp.where(one_hot, rank_order[None, :], 0), axis=1)
    owner = (owner + (outer - z) * inner * cores) % ranks
    target = owner * share + (position // period) * 2 + (stripe >= ranks).astype(jnp.int32)
    return target.reshape(1, count)


def local(video_tokens, conv_weight, point_weight, depth_weight, proj_weight, rank_order):
    frames, height, across, channels = video_tokens.shape
    cores, along = lax.axis_size("rows"), lax.axis_size("tm")
    paired = video_tokens.reshape(frames, height // 2, 2, across, channels)
    edges, pieces = cut(proj_weight, paired)
    up = lax.ppermute(edges[-1], "rows", [(i, (i + 1) % cores) for i in range(cores)])
    down = up
    if len(edges) > 1:
        down = lax.ppermute(edges[0], "rows", [((i + 1) % cores, i) for i in range(cores)])
    levels = spread_weight(pieces, frames // 2 * (height // 2) * (across // 2))
    shared = (paired, up, down, conv_weight, point_weight, depth_weight)
    sums, rims = [], []
    for o in reversed(range(frames // 2)):
        sent, kept = block_call(2 * o + 1, *shared)
        rims.insert(0, sent)
        sums.insert(0, block_call(2 * o, *shared, kept))
    rim = lax.ppermute(rims[-1], "tm", [(i, (i + 1) % along) for i in range(along)])
    if frames > 2:
        rim = jnp.concatenate([rim] + rims[:-1], axis=0)
    total = sums[0] if len(sums) == 1 else jnp.concatenate(sums, axis=0)
    placed = place_call(frames // 2, total, rim, slots(rank_order, total.shape[0]))
    return deliver(placed, levels)


def solution(mesh):
    return jax.shard_map(
        local,
        mesh=mesh,
        in_specs=(
            P(("groups", "tm"), "rows", None, None),
            P(),
            P(),
            P(),
            P(("tm", "rows"), None),
            P("groups"),
        ),
        out_specs=P(("groups", "tm", "rows"), None),
        check_vma=False,
    )
```
